32 devices in a mesh: parts: 2 (over y), mesh: 4 (over z), tile: 2 (over x), feat: 2 (over core).
Axes of the slice: x: 2, y: 2, z: 4, core: 2. Of those that a mesh axis runs over, the one named last changes fastest.
Arguments:
- fields: bfloat16 [2048, 128], P(('parts', 'mesh', 'tile')), parts along dimension 0, may hold values from -6 to 6
- owner_group: int32 [1024, 1], P(('mesh', 'tile')), may hold values from 0 to 7; in each aligned block of 128 rows (0 to 127, 128 to 255, ...) at most 32 rows name the same one
- owner_node: int32 [1024], P(('mesh', 'tile')), may hold values from 0 to 31
- stencil_codes: int32 [256, 8], P(('mesh', 'tile')), may hold values from 0 to 24
- coarse_ids: int32 [256], P(('mesh', 'tile')), may hold values from 0 to 15
- encode_weight: bfloat16 [128, 512], P(None, 'feat'), may hold values from -0.5 to 0.5
- process_weight: bfloat16 [512, 512], P(None, 'feat'), may hold values from -0.09375 to 0.09375
- coarse_weight: bfloat16 [512, 512], P(None, 'feat'), may hold values from -0.0625 to 0.0625
- decode_weight: bfloat16 [512, 128], P('feat'), may hold values from -0.25 to 0.25
- cotangent: float32 [2048, 128], P(('parts', 'mesh', 'tile')), parts along dimension 0, may hold values from -6 to 6
Outputs:
- prediction: float32 [2048, 128], P(('parts', 'mesh', 'tile')), parts along dimension 0
- encode_grad: float32 [256, 512], P('parts', 'feat'), parts along dimension 0
- process_grad: float32 [1024, 512], P('parts', 'feat'), parts along dimension 0
- coarse_grad: float32 [1024, 512], P('parts', 'feat'), parts along dimension 0
- decode_grad: float32 [1024, 128], P(('parts', 'feat')), parts along dimension 0
The draws below stay inside these ranges and needn't reach their ends.
There are 2 independent parts, one for each index of `parts`. The reference program is written for one: setup_inputs(seed, part) draws one part's arguments, and reference() takes and returns one part's arrays. A program takes and returns all parts, laid end to end along the dimension named above; an argument that names none is the same for every part. Nothing has to cross between parts.
Inputs may be any that keep to these rules, and one draw needn't show every extreme that they name: `owner_group`: in the rows of one device group no value is named more than 32 times.
All inputs are finite; a program needn't handle non-finite values.
Results may differ from the reference program's by a relative error of at most 0.0073.
Values may be sent and summed in bfloat16 or wider, within the bound.
No kernel may reach another device: no remote copies, remote signals or barrier semaphores. Data moves between devices by JAX's collectives and lax.ppermute only.
A program may use at most 64 MiB of HBM per device.

```python
import math
import jax
import jax.numpy as jnp
import numpy as np
from jax import lax

H = 512
C_IN = 128
C_OUT = 128
GB = 128
MA = 4
MB = 8
K = 8
CPD = 2
CAP = 32
GRID = 1024
NODES = 256
NC = 16
N_MESH = 4
N_TILE = 2


def draw_coarse_ids(key, part):
    key_near, key_far, key_pick = jax.random.split(jax.random.fold_in(key, 17), 3)
    owner_block = jnp.arange(NODES, dtype=jnp.int32) // (MA * MB)
    nearby = (owner_block * CPD + jax.random.randint(key_near, (NODES,), 0, 2 * CPD)) % NC
    anywhere = jax.random.randint(key_far, (NODES,), 0, NC)
    choose = jax.random.randint(key_pick, (NODES,), 0, 2)
    return jnp.where(choose == 0, nearby, anywhere).astype(jnp.int32)


def touch_ends(result, key, smallest, high):
    place = [jax.random.randint(jax.random.fold_in(key, axis), (), 0, length) for axis, length in enumerate(result.shape)]
    main_axis = result.shape.index(max(result.shape))
    beside = place[:main_axis] + [(place[main_axis] + 1) % result.shape[main_axis]] + place[main_axis + 1:]
    return result.at[tuple(place)].set(smallest).at[tuple(beside)].set(high)


def steps_of(key, extent, cuts, least, high):
    gain, own = 1.0, jax.random.fold_in(key, 6)
    for position, shards_of in cuts:
        steps = jnp.exp(jax.random.uniform(jax.random.fold_in(own, position), (shards_of,), jnp.float32, least / len(cuts), high / len(cuts)))
        gain = gain * jnp.repeat(steps, extent[position] // shards_of).reshape([-1 if axis == position else 1 for axis in range(len(extent))])
    return gain


def shared_out(stream_key, own, number, rows, count, top, bound, slope):
    ranking = jax.random.permutation(stream_key, count)
    packed, common = shares(count, rows * top, bound, slope, True), shares(count, rows * top, bound, slope, False)
    places = jnp.arange(count)

    def named(tallies, offset_by):
        used = int((tallies > 0).sum())
        fixed = max(1, used // 4)
        passed = fixed + (places - fixed + offset_by * (used - fixed)) % max(1, count - fixed)
        return jnp.zeros((count,), jnp.int32).at[ranking[jnp.where(places < fixed, places, passed)]].set(jnp.asarray(tallies, jnp.int32))

    tallies = jnp.where(number % 4 == 0, named(packed, number // 4), named(common, number - number // 4 - 1))
    mixed = jax.random.permutation(jax.random.fold_in(own, 3), count)
    giver, sink = mixed[0:count // 2 * 2:2], mixed[1:count // 2 * 2:2]
    margin = jnp.minimum(tallies[giver] - 1, bound - tallies[sink]) // 2
    margin = jnp.where((giver == ranking[0]) | (sink == ranking[0]) | (tallies[sink] == 0), 0, jnp.maximum(margin, 0))
    passed = jax.random.randint(jax.random.fold_in(own, 4), (count // 2,), 0, 1 << 20) % (margin + 1)
    tallies = tallies.at[giver].add(-passed).at[sink].add(passed)
    members = jnp.searchsorted(jnp.cumsum(tallies), jnp.arange(rows * top), side="right").astype(jnp.int32)
    grid = members.reshape(top, rows).T
    grid = grid[jax.random.permutation(jax.random.fold_in(own, 1), rows)]
    offset_by = jax.random.randint(jax.random.fold_in(own, 2), (rows, 1), 0, top)
    return jnp.take_along_axis(grid, (jnp.arange(top)[None, :] + offset_by) % top, axis=1)


def shares(count, total, reach, skew, full):
    loads = [(1 << 20) // math.isqrt(standing ** skew) + 1 for standing in range(1, count + 1)]
    largest = reach if full else min(reach, max(-(-total // count), total * loads[0] // sum(loads)))
    least = 1 if total - largest >= count - 1 else 0
    given, spare = [largest] + [least] * (count - 1), total - largest - least * (count - 1)
    while spare > 0:
        movable = [i for i in range(1, count) if given[i] < largest] or [i for i in range(1, count) if given[i] < reach]
        whole, left = sum([loads[i] for i in movable]), spare
        for i in movable:
            more = min(reach - given[i], max(1, left * loads[i] // whole), spare)
            given[i] = given[i] + more
            spare = spare - more
    return np.array(given)


def centred(key, dims, scale, bound, cuts=(), kind=jnp.bfloat16):
    drawn = jax.random.normal(key, dims, jnp.float32) * scale
    if len(cuts) > 0:
        drawn = steps_of(key, dims, cuts, -0.22, 0.18) * drawn
    return jnp.clip(drawn, min=-bound, max=bound).astype(kind)


def setup_inputs(seed: int = 0, part: int = 0) -> dict:
    key_of = jax.random.split(jax.random.key(seed), 11)
    part_splits = jax.random.split(jax.random.fold_in(key_of[10], part), 11)
    fields = centred(part_splits[0], (GRID, C_IN), 1.0, 6.0, ((0, 8),))
    owner_group_keys = jax.random.split(jax.random.fold_in(key_of[1], 1), GRID // GB)
    owner_group_turns = jax.random.permutation(jax.random.fold_in(key_of[1], 3), GRID // GB)
    owner_group = jax.vmap(lambda own, number: shared_out(jax.random.fold_in(key_of[1], 2), own, number, GB, N_MESH * N_TILE, 1, CAP, 2))(owner_group_keys, owner_group_turns).reshape((GRID, 1))
    owner_node = touch_ends(jax.random.randint(key_of[2], (GRID,), 0, MA * MB), jax.random.fold_in(key_of[2], 1), 0, (MA * MB) - 1).astype(jnp.int32)
    stencil_codes = touch_ends(jax.random.randint(key_of[3], (NODES, K), 0, 25), jax.random.fold_in(key_of[3], 1), 0, 24).astype(jnp.int32)
    coarse_ids = draw_coarse_ids(jax.random.fold_in(key_of[10], 71), part)
    encode_weight = centred(key_of[5], (C_IN, H), C_IN ** -0.5, 0.5, ((1, 2),))
    process_weight = centred(key_of[6], (H, H), (H * K) ** -0.5, 0.09375, ((1, 2),))
    coarse_weight = centred(key_of[7], (H, H), (H * MA * MB // CPD) ** -0.5, 0.0625, ((1, 2),))
    decode_weight = centred(key_of[8], (H, C_OUT), H ** -0.5, 0.25, ((0, 2),))
    cotangent = centred(part_splits[9], (GRID, C_OUT), 1.0, 6.0, ((0, 8),), jnp.float32)
    return {"fields": fields, "owner_group": owner_group, "owner_node": owner_node, "stencil_codes": stencil_codes, "coarse_ids": coarse_ids, "encode_weight": encode_weight, "process_weight": process_weight, "coarse_weight": coarse_weight, "decode_weight": decode_weight, "cotangent": cotangent}


def silu_grad(pre):
    sig = jax.nn.sigmoid(pre)
    return sig * (1.0 + pre * (1.0 - sig))

def to_torus(values):
    width_last = values.shape[-1]
    shaped = values.reshape(N_MESH, N_TILE, MA, MB, width_last)
    return jnp.transpose(shaped, (0, 2, 1, 3, 4)).reshape(N_MESH * MA, N_TILE * MB, width_last)

def from_torus(values):
    width_last = values.shape[-1]
    shaped = values.reshape(N_MESH, MA, N_TILE, MB, width_last)
    return jnp.transpose(shaped, (0, 2, 1, 3, 4)).reshape(NODES, width_last)

def reference(fields, owner_group, owner_node, stencil_codes, coarse_ids, encode_weight, process_weight, coarse_weight, decode_weight, cotangent):
    highest = lax.Precision.HIGHEST
    target = (owner_group[:, 0] * (MA * MB) + owner_node).astype(jnp.int32)
    pre_encode = jnp.dot(fields, encode_weight, preferred_element_type=jnp.float32)
    hidden = jax.nn.silu(pre_encode).astype(jnp.bfloat16)
    node_in = jax.ops.segment_sum(hidden.astype(jnp.float32), target, NODES).astype(jnp.bfloat16)
    counts = lax.optimization_barrier(jnp.sum((stencil_codes[:, :, None] == jnp.arange(25, dtype=jnp.int32)[None, None, :]).astype(jnp.float32), axis=1))
    count_grid = to_torus(counts)
    node_grid = to_torus(node_in.astype(jnp.float32))
    gathered = jnp.zeros(node_grid.shape, jnp.float32)
    for code_index in range(25):
        step_x = code_index // 5 - 2
        step_y = code_index % 5 - 2
        gathered = gathered + count_grid[:, :, code_index:code_index + 1] * jnp.roll(node_grid, (-step_x, -step_y), axis=(0, 1))
    agg = from_torus(gathered).astype(jnp.bfloat16)
    pre_mesh = jnp.dot(agg, process_weight, preferred_element_type=jnp.float32)
    level_one = node_in.astype(jnp.float32) + jax.nn.silu(pre_mesh)
    coarse_in = jax.ops.segment_sum(level_one, coarse_ids, NC).astype(jnp.bfloat16)
    pre_coarse = jnp.dot(coarse_in, coarse_weight, preferred_element_type=jnp.float32)
    coarse_out = jax.nn.silu(pre_coarse).astype(jnp.bfloat16)
    level_two = (level_one + coarse_out.astype(jnp.float32)[coarse_ids]).astype(jnp.bfloat16)
    merged = (hidden.astype(jnp.float32) + level_two.astype(jnp.float32)[target]).astype(jnp.bfloat16)
    prediction = jnp.dot(merged, decode_weight, preferred_element_type=jnp.float32)
    decode_grad = jnp.dot(merged.astype(jnp.float32).T, cotangent, precision=highest)
    grad_merged = jnp.dot(cotangent, decode_weight.astype(jnp.float32).T, precision=highest)
    grad_rows = grad_merged.astype(jnp.bfloat16)
    grad_two = jax.ops.segment_sum(grad_rows.astype(jnp.float32), target, NODES)
    grad_coarse_out = jax.ops.segment_sum(grad_two, coarse_ids, NC)
    grad_pre_coarse = grad_coarse_out * silu_grad(pre_coarse)
    coarse_grad = jnp.dot(coarse_in.astype(jnp.float32).T, grad_pre_coarse, precision=highest)
    grad_coarse_in = jnp.dot(grad_pre_coarse, coarse_weight.astype(jnp.float32).T, precision=highest)
    grad_one = grad_two + grad_coarse_in[coarse_ids]
    grad_pre_mesh = grad_one * silu_grad(pre_mesh)
    process_grad = jnp.dot(agg.astype(jnp.float32).T, grad_pre_mesh, precision=highest)
    grad_agg = jnp.dot(grad_pre_mesh, process_weight.astype(jnp.float32).T, precision=highest).astype(jnp.bfloat16)
    grad_grid = to_torus(grad_agg.astype(jnp.float32))
    spread = jnp.zeros(grad_grid.shape, jnp.float32)
    for code_index in range(25):
        step_x = code_index // 5 - 2
        step_y = code_index % 5 - 2
        spread = spread + jnp.roll(count_grid[:, :, code_index:code_index + 1] * grad_grid, (step_x, step_y), axis=(0, 1))
    grad_zero = (grad_one + from_torus(spread)).astype(jnp.bfloat16)
    grad_hidden = grad_merged + grad_zero.astype(jnp.float32)[target]
    grad_pre_encode = grad_hidden * silu_grad(pre_encode)
    encode_grad = jnp.dot(fields.astype(jnp.float32).T, grad_pre_encode, precision=highest)
    return (prediction, encode_grad, process_grad, coarse_grad, decode_grad)
```

```python
import functools

import jax
import jax.numpy as jnp
from jax import lax
from jax.experimental import pallas as pl
from jax.experimental.pallas import tpu as pltpu
from jax.sharding import PartitionSpec as P

MA = 4
MB = 8
CPD = 2
ID_ROWS = 16
REPLICATE_LIMIT = 1 << 20

F32 = jnp.float32
BF16 = jnp.bfloat16
NN = (((1,), (0,)), ((), ()))
NT = (((1,), (1,)), ((), ()))
TN = (((0,), (0,)), ((), ()))


def mm(lhs, rhs, dims=NN):
    return lax.dot_general(lhs, rhs, dims, preferred_element_type=F32)


def split(value):
    high = value.astype(BF16)
    return high, (value - high.astype(F32)).astype(BF16)


def pack_kernel(fields, group_col, node_row, codes, coarse_row, cotangent, out, wide):
    rows = fields.shape[0]
    local, degree = codes.shape
    core = lax.axis_index("feat")

    @pl.when(core == 0)
    def _():
        out[0:rows, :] = fields[...]

    @pl.when(core != 0)
    def _():
        out[0:rows, :] = cotangent[...].astype(BF16)

    wide[...] = jnp.zeros(wide.shape, F32)
    wide[:, 0:1] = group_col[...].astype(F32)
    wide[0:local, 2 : 2 + degree] = codes[...].astype(F32)
    turned = jnp.transpose(wide[...])
    wide[0:ID_ROWS, :] = turned[0:ID_ROWS, :]
    wide[1:2, :] = node_row[...].astype(F32)
    wide[2 + degree : 3 + degree, 0:local] = coarse_row[...].astype(F32)
    out[rows : rows + ID_ROWS, :] = wide[0:ID_ROWS, :].astype(BF16)


def step_kernel(
    mesh_count,
    tile_count,
    degree,
    near,
    far,
    we_own,
    wp_own,
    wc_own,
    wd_own,
    we_oth,
    wp_oth,
    wc_oth,
    wd_oth,
    prediction,
    encode_grad,
    process_grad,
    coarse_grad,
    decode_grad,
    cells,
    cots,
    hid,
    slope,
    hit,
    hit_t,
    ids,
    gpe,
):
    groups = mesh_count * tile_count
    local = MA * MB
    nodes = groups * local
    block = near.shape[0] // groups
    rows = block - ID_ROWS
    width = we_own.shape[1]
    core = lax.axis_index("feat")
    my_mesh = lax.axis_index("mesh")
    my_tile = lax.axis_index("tile")
    own = pl.ds(pl.multiple_of(core * width, width), width)
    oth = pl.ds(pl.multiple_of((1 - core) * width, width), width)
    sub = lax.broadcasted_iota(jnp.int32, (nodes, rows), 0).astype(F32)
    lane = lax.broadcasted_iota(jnp.int32, (rows, nodes), 1).astype(F32)
    for p in range(groups):
        far_tile, shift = p // mesh_count, p % mesh_count
        group = lax.rem(my_mesh - shift + mesh_count, mesh_count) * tile_count + lax.rem(
            my_tile - far_tile + tile_count, tile_count
        )
        here = pl.ds(p * block, rows)
        span = slice(p * rows, (p + 1) * rows)
        a, b = near[here, :], far[here, :]
        cell = jnp.where(core == 0, a, b)
        cells[span, :] = cell
        cots[span, :] = jnp.where(core == 0, b, a)
        tags = near[pl.ds(p * block + rows, ID_ROWS), :].astype(F32)
        tags_t = jnp.transpose(tags)
        hit[:, span] = (sub == tags[0:1, :] * local + tags[1:2, :]).astype(BF16)
        hit_t[span, :] = (lane == tags_t[:, 0:1] * local + tags_t[:, 1:2]).astype(BF16)
        ids[pl.ds(pl.multiple_of(group * local, local), local), :] = tags_t[0:local, :]
        pre = mm(cell, we_own[...])
        sig = jax.nn.sigmoid(pre)
        act = pre * sig
        hid[span, 0:width] = act.astype(BF16)
        slope[span, :] = sig + act * (1.0 - sig)
        pre = mm(cell, we_oth[...])
        hid[span, width:] = (pre * jax.nn.sigmoid(pre)).astype(BF16)

    tags = ids[...].astype(jnp.int32)
    index = lax.broadcasted_iota(jnp.int32, (nodes, ID_ROWS), 0)
    group, place = lax.div(index, local), lax.rem(index, local)
    row = lax.div(group, tile_count) * MA + lax.div(place, MB)
    col = lax.rem(group, tile_count) * MB + lax.rem(place, MB)
    tall, broad = mesh_count * MA, tile_count * MB
    row = lax.rem(row + lax.div(tags, 5) - 2 + tall, tall)
    col = lax.rem(col + lax.rem(tags, 5) - 2 + broad, broad)
    peer = (lax.div(row, MA) * tile_count + lax.div(col, MB)) * local
    peer = peer + lax.rem(row, MA) * MB + lax.rem(col, MB)
    over = lax.broadcasted_iota(jnp.int32, (nodes, nodes), 1)
    reach = jnp.zeros((nodes, nodes), F32)
    for k in range(2, 2 + degree):
        reach = reach + (over == peer[:, k : k + 1]).astype(F32)
    reach = reach.astype(BF16)
    coarse_count = CPD * groups
    member = (
        lax.broadcasted_iota(jnp.int32, (nodes, coarse_count), 1)
        == tags[:, 2 + degree : 3 + degree]
    ).astype(BF16)

    node_in = mm(hit[...], hid[...]).astype(BF16)
    agg = mm(reach, node_in).astype(BF16)
    agg_own, agg_oth = agg[:, :width], agg[:, width:]
    pre_mesh = (
        mm(agg_own, wp_own[own, :]) + mm(agg_oth, wp_own[oth, :]),
        mm(agg_own, wp_oth[own, :]) + mm(agg_oth, wp_oth[oth, :]),
    )
    sig_mesh = tuple(jax.nn.sigmoid(v) for v in pre_mesh)
    act_mesh = tuple(v * s for v, s in zip(pre_mesh, sig_mesh))
    level_one = (
        node_in[:, :width].astype(F32) + act_mesh[0],
        node_in[:, width:].astype(F32) + act_mesh[1],
    )
    coarse_in = []
    for v in level_one:
        high, low = split(v)
        coarse_in.append((mm(member, high, TN) + mm(member, low, TN)).astype(BF16))
    pre_coarse = (
        mm(coarse_in[0], wc_own[own, :]) + mm(coarse_in[1], wc_own[oth, :]),
        mm(coarse_in[0], wc_oth[own, :]) + mm(coarse_in[1], wc_oth[oth, :]),
    )
    sig_coarse = tuple(jax.nn.sigmoid(v) for v in pre_coarse)
    act_coarse = tuple(v * s for v, s in zip(pre_coarse, sig_coarse))
    level_two = tuple(
        (v + mm(member, c.astype(BF16))).astype(BF16) for v, c in zip(level_one, act_coarse)
    )
    mine = hit_t[0:rows, :]
    merged = (
        (hid[0:rows, :width].astype(F32) + mm(mine, level_two[0])).astype(BF16),
        (hid[0:rows, width:].astype(F32) + mm(mine, level_two[1])).astype(BF16),
    )
    prediction[...] = mm(merged[0], wd_own[...]) + mm(merged[1], wd_oth[...])

    cot = cots[...]
    node_cot = mm(hit[...], cot)
    cot_high, cot_low = split(node_cot)
    decode_grad[...] = mm(hid[:, :width], cot, TN) + mm(level_two[0], cot_high, TN)
    grad_two = tuple(mm(cot_high, w[...], NT) + mm(cot_low, w[...], NT) for w in (wd_own, wd_oth))
    grad_pre_coarse = []
    for g, s, c in zip(grad_two, sig_coarse, act_coarse):
        high, low = split(g)
        total = mm(member, high, TN) + mm(member, low, TN)
        grad_pre_coarse.append(total * (s + c * (1.0 - s)))
    gpc = [v.astype(BF16) for v in grad_pre_coarse]
    coarse_grad[own, :] = mm(coarse_in[0], gpc[0], TN)
    coarse_grad[oth, :] = mm(coarse_in[1], gpc[0], TN)
    grad_coarse_in = (
        mm(gpc[0], wc_own[own, :], NT) + mm(gpc[1], wc_oth[own, :], NT),
        mm(gpc[0], wc_own[oth, :], NT) + mm(gpc[1], wc_oth[oth, :], NT),
    )
    grad_one = tuple(g + mm(member, c.astype(BF16)) for g, c in zip(grad_two, grad_coarse_in))
    gpm = tuple(
        (g * (s + c * (1.0 - s))).astype(BF16) for g, s, c in zip(grad_one, sig_mesh, act_mesh)
    )
    process_grad[own, :] = mm(agg_own, gpm[0], TN)
    process_grad[oth, :] = mm(agg_oth, gpm[0], TN)
    grad_agg = (mm(gpm[0], wp_own[own, :], NT) + mm(gpm[1], wp_oth[own, :], NT)).astype(BF16)
    grad_zero = (grad_one[0] + mm(reach, grad_agg, TN)).astype(BF16)
    for p in range(groups):
        span = slice(p * rows, (p + 1) * rows)
        grad_hidden = mm(cots[span, :], wd_own[...], NT) + mm(hit_t[span, :], grad_zero)
        gpe[span, :] = (grad_hidden * slope[span, :]).astype(BF16)
    encode_grad[...] = mm(cells[...], gpe[...], TN)


def replicated(
    fields,
    owner_group,
    owner_node,
    stencil_codes,
    coarse_ids,
    encode_weight,
    process_weight,
    coarse_weight,
    decode_weight,
    cotangent,
):
    mesh_count = lax.axis_size("mesh")
    tile_count = lax.axis_size("tile")
    groups = mesh_count * tile_count
    rows, c_in = fields.shape
    c_out = cotangent.shape[1]
    width = encode_weight.shape[1]
    nodes = groups * MA * MB
    block = rows + ID_ROWS
    weights = (encode_weight, process_weight, coarse_weight, decode_weight)
    swap = [(0, 1), (1, 0)]
    others = tuple(lax.ppermute(w, "feat", swap) for w in weights)
    payload = pl.pallas_call(
        pack_kernel,
        out_shape=jax.ShapeDtypeStruct((block, c_in), BF16),
        scratch_shapes=[pltpu.VMEM((rows, c_in), F32)],
    )(
        fields,
        owner_group,
        owner_node.reshape(1, rows),
        stencil_codes,
        coarse_ids.reshape(1, MA * MB),
        cotangent,
    )
    blocks = [payload]
    for shift in range(1, mesh_count):
        ring = [(i, (i + shift) % mesh_count) for i in range(mesh_count)]
        blocks.append(lax.ppermute(payload, "mesh", ring))
    column = jnp.concatenate(blocks, axis=0)
    columns = [column]
    for shift in range(1, tile_count):
        ring = [(i, (i + shift) % tile_count) for i in range(tile_count)]
        columns.append(lax.ppermute(column, "tile", ring))
    near = jnp.concatenate(columns, axis=0)
    far = lax.ppermute(near, "feat", swap)
    cells = groups * rows
    return pl.pallas_call(
        functools.partial(step_kernel, mesh_count, tile_count, stencil_codes.shape[1]),
        out_shape=(
            jax.ShapeDtypeStruct((rows, c_out), F32),
            jax.ShapeDtypeStruct((c_in, width), F32),
            jax.ShapeDtypeStruct(process_weight.shape, F32),
            jax.ShapeDtypeStruct(coarse_weight.shape, F32),
            jax.ShapeDtypeStruct((width, c_out), F32),
        ),
        scratch_shapes=[
            pltpu.VMEM((cells, c_in), BF16),
            pltpu.VMEM((cells, c_out), BF16),
            pltpu.VMEM((cells, 2 * width), BF16),
            pltpu.VMEM((cells, width), F32),
            pltpu.VMEM((nodes, cells), BF16),
            pltpu.VMEM((cells, nodes), BF16),
            pltpu.VMEM((nodes, ID_ROWS), F32),
            pltpu.VMEM((cells, width), BF16),
        ],
    )(near, far, *weights, *others)


def padded(array, sides, width):
    for axis, dim in sides:
        peers, length = (lax.axis_size(axis), array.shape[dim])
        up = [(i, (i + 1) % peers) for i in range(peers)]
        down = [(j, i) for i, j in up]
        last = lax.slice_in_dim(array, length - width, length, axis=dim)
        initial = lax.slice_in_dim(array, 0, width, axis=dim)
        before = lax.ppermute(last, axis, up)
        after = lax.ppermute(initial, axis, down)
        array = jnp.concatenate([before, array, after], axis=dim)
    return array


def silu_grad(pre):
    sig = jax.nn.sigmoid(pre)
    return sig * (1.0 + pre * (1.0 - sig))


def send_rows(outgoing, slot_node):
    feat_width = outgoing.shape[-1]
    got, got_node = (
        lax.all_to_all(outgoing, ("mesh", "tile"), split_axis=0, concat_axis=0, tiled=True),
        lax.all_to_all(slot_node, ("mesh", "tile"), split_axis=0, concat_axis=0, tiled=True),
    )
    return (got.reshape(-1, feat_width), got_node.reshape(-1))


def route_block(block, mesh_count, tile_count, purpose):
    feat_width = block.shape[-1]
    slot_count = block.shape[0] // (mesh_count * tile_count)
    flat_shape = (mesh_count * tile_count, slot_count, feat_width)
    if purpose == "reply":
        moved = lax.all_to_all(
            block.reshape(flat_shape), ("mesh", "tile"), split_axis=0, concat_axis=0, tiled=True
        )
    elif purpose == "gradient":
        moved = lax.all_to_all(
            block.reshape(flat_shape), ("mesh", "tile"), split_axis=0, concat_axis=0, tiled=True
        )
    else:
        moved = lax.all_to_all(
            block.reshape(flat_shape), ("mesh", "tile"), split_axis=0, concat_axis=0, tiled=True
        )
    return moved.reshape(-1, feat_width)


def distributed(
    fields,
    owner_group,
    owner_node,
    stencil_codes,
    coarse_ids,
    encode_weight,
    process_weight,
    coarse_weight,
    decode_weight,
    cotangent,
):
    highest = lax.Precision.HIGHEST
    row_count = fields.shape[0]
    mesh_count = lax.axis_size("mesh")
    tile_count = lax.axis_size("tile")
    groups = mesh_count * tile_count
    slot_count = 2 * row_count // groups
    feat_width = encode_weight.shape[1]
    patch_rows = MA
    patch_cols = MB
    nodes_local = patch_rows * patch_cols
    coarse_count = CPD * groups
    target = owner_group[:, 0]
    group_onehot = (target[:, None] == jnp.arange(groups, dtype=jnp.int32)[None, :]).astype(
        jnp.int32
    )
    earlier = jnp.cumsum(group_onehot, axis=0) - group_onehot
    position = target * slot_count + jnp.sum(earlier * group_onehot, axis=1)
    matches = jnp.arange(groups * slot_count, dtype=jnp.int32)[:, None] == position[None, :]
    dispatch = matches.astype(jnp.bfloat16)
    slot_node = (jnp.max(jnp.where(matches, owner_node[None, :] + 1, 0), axis=1) - 1).reshape(
        groups, slot_count
    )
    pre_encode = jnp.dot(fields, encode_weight, preferred_element_type=jnp.float32)
    hidden = jax.nn.silu(pre_encode).astype(jnp.bfloat16)
    outgoing = jnp.dot(dispatch, hidden, preferred_element_type=jnp.float32).astype(jnp.bfloat16)
    incoming, incoming_node = send_rows(outgoing.reshape(groups, slot_count, feat_width), slot_node)
    node_match = (
        incoming_node[:, None] == jnp.arange(nodes_local, dtype=jnp.int32)[None, :]
    ).astype(jnp.bfloat16)
    node_in = jnp.einsum(
        "sn,sh->nh", node_match, incoming, preferred_element_type=jnp.float32
    ).astype(jnp.bfloat16)
    counts = jnp.sum(
        (stencil_codes[:, :, None] == jnp.arange(25, dtype=jnp.int32)[None, None, :]).astype(
            jnp.float32
        ),
        axis=1,
    )
    counts = counts.astype(jnp.bfloat16).reshape(patch_rows, patch_cols, 25)
    padded_nodes, padded_counts = (
        padded(node_in.reshape(patch_rows, patch_cols, feat_width), (("mesh", 0), ("tile", 1)), 2),
        padded(counts, (("mesh", 0), ("tile", 1)), 2),
    )
    gathered = jnp.zeros((patch_rows, patch_cols, feat_width), jnp.float32)
    for code_index in range(25):
        step_x = code_index // 5 - 2
        step_y = code_index % 5 - 2
        weight_here = padded_counts[
            2 : 2 + patch_rows, 2 : 2 + patch_cols, code_index : code_index + 1
        ].astype(jnp.float32)
        gathered = gathered + weight_here * padded_nodes[
            2 + step_x : 2 + step_x + patch_rows, 2 + step_y : 2 + step_y + patch_cols
        ].astype(jnp.float32)
    agg = gathered.reshape(nodes_local, feat_width).astype(jnp.bfloat16)
    agg_full = lax.all_gather(agg, "feat", axis=1, tiled=True)
    pre_mesh = jnp.dot(agg_full, process_weight, preferred_element_type=jnp.float32)
    level_one = node_in.astype(jnp.float32) + jax.nn.silu(pre_mesh)
    coarse_match = (
        coarse_ids[:, None] == jnp.arange(coarse_count, dtype=jnp.int32)[None, :]
    ).astype(jnp.float32)
    coarse_part = jnp.dot(coarse_match.T, level_one, precision=highest)
    coarse_total = lax.psum(coarse_part, ("mesh", "tile"))
    coarse_in = lax.all_gather(coarse_total.astype(jnp.bfloat16), "feat", axis=1, tiled=True)
    pre_coarse = jnp.dot(coarse_in, coarse_weight, preferred_element_type=jnp.float32)
    coarse_out = jax.nn.silu(pre_coarse).astype(jnp.bfloat16)
    level_two = (
        level_one
        + jnp.dot(coarse_match.astype(jnp.bfloat16), coarse_out, preferred_element_type=jnp.float32)
    ).astype(jnp.bfloat16)
    reply_rows = jnp.dot(node_match, level_two, preferred_element_type=jnp.float32).astype(
        jnp.bfloat16
    )
    returned = route_block(reply_rows, mesh_count, tile_count, "reply")
    merged = (
        hidden.astype(jnp.float32)
        + jnp.einsum("sr,sh->rh", dispatch, returned, preferred_element_type=jnp.float32)
    ).astype(jnp.bfloat16)
    pred_part = jnp.dot(merged, decode_weight, preferred_element_type=jnp.float32)
    prediction = lax.psum(pred_part, "feat")
    decode_grad = jnp.dot(merged.astype(jnp.float32).T, cotangent, precision=highest)
    grad_merged = jnp.dot(cotangent, decode_weight.astype(jnp.float32).T, precision=highest)
    grad_out = jnp.dot(
        dispatch, grad_merged.astype(jnp.bfloat16), preferred_element_type=jnp.float32
    ).astype(jnp.bfloat16)
    grad_in = route_block(grad_out, mesh_count, tile_count, "gradient")
    grad_two = jnp.einsum("sn,sh->nh", node_match, grad_in, preferred_element_type=jnp.float32)
    coarse_grad_part = jnp.dot(coarse_match.T, grad_two, precision=highest)
    grad_coarse_out = lax.psum(coarse_grad_part, ("mesh", "tile"))
    grad_pre_coarse = grad_coarse_out * silu_grad(pre_coarse)
    coarse_grad = jnp.dot(coarse_in.astype(jnp.float32).T, grad_pre_coarse, precision=highest)
    grad_coarse_full = jnp.dot(
        grad_pre_coarse, coarse_weight.astype(jnp.float32).T, precision=highest
    )
    grad_coarse_in = lax.psum_scatter(grad_coarse_full, "feat", scatter_dimension=1, tiled=True)
    grad_one = grad_two + jnp.dot(coarse_match, grad_coarse_in, precision=highest)
    grad_pre_mesh = grad_one * silu_grad(pre_mesh)
    process_grad = jnp.dot(agg_full.astype(jnp.float32).T, grad_pre_mesh, precision=highest)
    grad_pre_full = lax.all_gather(grad_pre_mesh, "feat", axis=1, tiled=True)
    weight_full = lax.all_gather(process_weight, "feat", axis=1, tiled=True)
    own_rows = lax.dynamic_slice_in_dim(
        weight_full, lax.axis_index("feat") * feat_width, feat_width, 0
    )
    grad_agg = jnp.dot(grad_pre_full, own_rows.astype(jnp.float32).T, precision=highest).astype(
        jnp.bfloat16
    )
    padded_grad = padded(
        grad_agg.reshape(patch_rows, patch_cols, feat_width), (("mesh", 0), ("tile", 1)), 2
    )
    spread = jnp.zeros((patch_rows, patch_cols, feat_width), jnp.float32)
    for code_index in range(25):
        step_x = code_index // 5 - 2
        step_y = code_index % 5 - 2
        weight_there = padded_counts[
            2 - step_x : 2 - step_x + patch_rows,
            2 - step_y : 2 - step_y + patch_cols,
            code_index : code_index + 1,
        ].astype(jnp.float32)
        spread = spread + weight_there * padded_grad[
            2 - step_x : 2 - step_x + patch_rows, 2 - step_y : 2 - step_y + patch_cols
        ].astype(jnp.float32)
    grad_zero = (grad_one + spread.reshape(nodes_local, feat_width)).astype(jnp.bfloat16)
    back_rows = jnp.dot(node_match, grad_zero, preferred_element_type=jnp.float32).astype(
        jnp.bfloat16
    )
    grad_back = route_block(back_rows, mesh_count, tile_count, "return")
    grad_hidden = grad_merged + jnp.einsum(
        "sr,sh->rh", dispatch, grad_back, preferred_element_type=jnp.float32
    )
    grad_pre_encode = grad_hidden * silu_grad(pre_encode)
    encode_grad = jnp.dot(fields.astype(jnp.float32).T, grad_pre_encode, precision=highest)
    encode_grad, process_grad, decode_grad = lax.psum(
        (encode_grad, process_grad, decode_grad), ("mesh", "tile")
    )
    return (prediction, encode_grad, process_grad, coarse_grad, decode_grad)


def body(fields, owner_group, owner_node, stencil_codes, *rest):
    groups = lax.axis_size("mesh") * lax.axis_size("tile")
    rows, c_in = fields.shape
    cells, nodes = groups * rows, groups * MA * MB
    degree = stencil_codes.shape[1]
    fits = (
        cells * nodes <= REPLICATE_LIMIT
        and lax.axis_size("feat") == 2
        and rows == c_in == rest[-1].shape[1]
        and max(nodes, 25) <= 256
        and degree + 3 <= ID_ROWS
        and MA * MB <= rows
    )
    plan = replicated if fits else distributed
    return plan(fields, owner_group, owner_node, stencil_codes, *rest)


def solution(mesh):
    placed = (
        P(("parts", "mesh", "tile"), None),
        P(("mesh", "tile"), None),
        P(("mesh", "tile")),
        P(("mesh", "tile"), None),
        P(("mesh", "tile")),
        P(None, "feat"),
        P(None, "feat"),
        P(None, "feat"),
        P("feat", None),
        P(("parts", "mesh", "tile"), None),
    )
    return jax.shard_map(
        body,
        mesh=mesh,
        in_specs=placed,
        out_specs=(
            P(("parts", "mesh", "tile"), None),
            P("parts", "feat"),
            P("parts", "feat"),
            P("parts", "feat"),
            P(("parts", "feat"), None),
        ),
        check_vma=False,
    )
```

```python
import functools

import jax
import jax.numpy as jnp
from jax import lax
from jax.experimental import pallas as pl
from jax.experimental.pallas import tpu as pltpu
from jax.sharding import PartitionSpec as P

MA = 4
MB = 8
CPD = 2
ID_ROWS = 16
REPLICATE_LIMIT = 1 << 20

F32 = jnp.float32
BF16 = jnp.bfloat16
NN = (((1,), (0,)), ((), ()))
NT = (((1,), (1,)), ((), ()))
TN = (((0,), (0,)), ((), ()))


def mm(lhs, rhs, dims=NN):
    return lax.dot_general(lhs, rhs, dims, preferred_element_type=F32)


def split(value):
    high = value.astype(BF16)
    return high, (value - high.astype(F32)).astype(BF16)


def held(value):
    return pltpu.with_memory_space_constraint(value, pltpu.VMEM)


def pack_kernel(fields, group_row, node_row, codes, coarse_row, cotangent, out, wide):
    rows = fields.shape[0]
    degree, local = codes.shape
    core = lax.axis_index("feat")

    @pl.when(core == 0)
    def _():
        out[0:rows, :] = fields[...]

    @pl.when(core != 0)
    def _():
        out[0:rows, :] = cotangent[...].astype(BF16)

    wide[...] = jnp.zeros(wide.shape, F32)
    wide[0:1, :] = group_row[...].astype(F32)
    wide[1:2, :] = node_row[...].astype(F32)
    wide[2 : 2 + degree, 0:local] = codes[...].astype(F32)
    wide[2 + degree : 3 + degree, 0:local] = coarse_row[...].astype(F32)
    out[rows : rows + ID_ROWS, :] = wide[...].astype(BF16)


def index_kernel(mesh_count, tile_count, degree, near, hit, hit_t, reach_out, member_out, ids):
    groups = mesh_count * tile_count
    local = MA * MB
    nodes = groups * local
    block = near.shape[0] // groups
    rows = block - ID_ROWS
    my_mesh = lax.axis_index("mesh")
    my_tile = lax.axis_index("tile")
    sub = lax.broadcasted_iota(jnp.int32, (nodes, rows), 0).astype(F32)
    lane = lax.broadcasted_iota(jnp.int32, (rows, nodes), 1).astype(F32)
    for p in range(groups):
        far_tile, shift = p // mesh_count, p % mesh_count
        group = lax.rem(my_mesh - shift + mesh_count, mesh_count) * tile_count + lax.rem(
            my_tile - far_tile + tile_count, tile_count
        )
        span = slice(p * rows, (p + 1) * rows)
        tags = near[pl.ds(p * block + rows, ID_ROWS), :].astype(F32)
        tags_t = jnp.transpose(tags)
        hit[:, span] = (sub == tags[0:1, :] * local + tags[1:2, :]).astype(BF16)
        hit_t[span, :] = (lane == tags_t[:, 0:1] * local + tags_t[:, 1:2]).astype(BF16)
        ids[pl.ds(pl.multiple_of(group * local, local), local), :] = tags_t[0:local, :]

    tags = ids[...].astype(jnp.int32)
    index = lax.broadcasted_iota(jnp.int32, (nodes, ID_ROWS), 0)
    group, place = lax.div(index, local), lax.rem(index, local)
    row = lax.div(group, tile_count) * MA + lax.div(place, MB)
    col = lax.rem(group, tile_count) * MB + lax.rem(place, MB)
    tall, broad = mesh_count * MA, tile_count * MB
    row = lax.rem(row + lax.div(tags, 5) - 2 + tall, tall)
    col = lax.rem(col + lax.rem(tags, 5) - 2 + broad, broad)
    peer = (lax.div(row, MA) * tile_count + lax.div(col, MB)) * local
    peer = peer + lax.rem(row, MA) * MB + lax.rem(col, MB)
    over = lax.broadcasted_iota(jnp.int32, (nodes, nodes), 1)
    reach = jnp.zeros((nodes, nodes), F32)
    for k in range(2, 2 + degree):
        reach = reach + (over == peer[:, k : k + 1]).astype(F32)
    reach_out[...] = reach.astype(BF16)
    member_out[...] = (
        lax.broadcasted_iota(jnp.int32, (nodes, CPD * groups), 1)
        == tags[:, 2 + degree : 3 + degree]
    ).astype(BF16)


def step_kernel(
    groups,
    near,
    far,
    hit,
    hit_t,
    reach_ref,
    member_ref,
    we_own,
    wp_own,
    wc_own,
    wd_own,
    we_oth,
    wp_oth,
    wc_oth,
    wd_oth,
    prediction_out,
    encode_out,
    process_out,
    coarse_out,
    decode_out,
    cells,
    cots,
    hid,
    slope,
    gpe,
    prediction,
    encode_grad,
    process_grad,
    coarse_grad,
    decode_grad,
    sems,
):
    block = near.shape[0] // groups
    rows = block - ID_ROWS
    width = we_own.shape[1]
    core = lax.axis_index("feat")
    own = pl.ds(pl.multiple_of(core * width, width), width)
    oth = pl.ds(pl.multiple_of((1 - core) * width, width), width)
    sent = [
        pltpu.make_async_copy(source, target, sems.at[i])
        for i, (source, target) in enumerate(
            (
                (prediction, prediction_out),
                (encode_grad, encode_out),
                (process_grad, process_out),
                (coarse_grad, coarse_out),
                (decode_grad, decode_out),
            )
        )
    ]
    for p in range(groups):
        here = pl.ds(p * block, rows)
        span = slice(p * rows, (p + 1) * rows)
        a, b = near[here, :], far[here, :]
        cell = jnp.where(core == 0, a, b)
        cells[span, :] = cell
        cots[span, :] = jnp.where(core == 0, b, a)
        pre = mm(cell, we_own[...])
        sig = jax.nn.sigmoid(pre)
        act = pre * sig
        hid[span, 0:width] = act.astype(BF16)
        slope[span, :] = sig + act * (1.0 - sig)
        pre = mm(cell, we_oth[...])
        hid[span, width:] = (pre * jax.nn.sigmoid(pre)).astype(BF16)

    reach = reach_ref[...]
    member = member_ref[...]
    node_in = mm(hit[...], hid[...]).astype(BF16)
    agg = mm(reach, node_in).astype(BF16)
    agg_own, agg_oth = agg[:, :width], agg[:, width:]
    pre_mesh = (
        mm(agg_own, wp_own[own, :]) + mm(agg_oth, wp_own[oth, :]),
        mm(agg_own, wp_oth[own, :]) + mm(agg_oth, wp_oth[oth, :]),
    )
    sig_mesh = tuple(jax.nn.sigmoid(v) for v in pre_mesh)
    act_mesh = tuple(v * s for v, s in zip(pre_mesh, sig_mesh))
    level_one = (
        node_in[:, :width].astype(F32) + act_mesh[0],
        node_in[:, width:].astype(F32) + act_mesh[1],
    )
    coarse_in = []
    for v in level_one:
        high, low = split(v)
        coarse_in.append((mm(member, high, TN) + mm(member, low, TN)).astype(BF16))
    pre_coarse = (
        mm(coarse_in[0], wc_own[own, :]) + mm(coarse_in[1], wc_own[oth, :]),
        mm(coarse_in[0], wc_oth[own, :]) + mm(coarse_in[1], wc_oth[oth, :]),
    )
    sig_coarse = tuple(jax.nn.sigmoid(v) for v in pre_coarse)
    act_coarse = tuple(v * s for v, s in zip(pre_coarse, sig_coarse))
    level_two = tuple(
        (v + mm(member, c.astype(BF16))).astype(BF16) for v, c in zip(level_one, act_coarse)
    )
    mine = hit_t[0:rows, :]
    merged = (
        (hid[0:rows, :width].astype(F32) + mm(mine, level_two[0])).astype(BF16),
        (hid[0:rows, width:].astype(F32) + mm(mine, level_two[1])).astype(BF16),
    )
    prediction[...] = mm(merged[0], wd_own[...]) + mm(merged[1], wd_oth[...])
    sent[0].start()

    cot = cots[...]
    node_cot = mm(hit[...], cot)
    cot_high, cot_low = split(node_cot)
    decode_grad[...] = mm(hid[:, :width], cot, TN) + mm(level_two[0], cot_high, TN)
    sent[4].start()
    grad_two = tuple(mm(cot_high, w[...], NT) + mm(cot_low, w[...], NT) for w in (wd_own, wd_oth))
    grad_pre_coarse = []
    for g, s, c in zip(grad_two, sig_coarse, act_coarse):
        high, low = split(g)
        total = mm(member, high, TN) + mm(member, low, TN)
        grad_pre_coarse.append(total * (s + c * (1.0 - s)))
    gpc = [v.astype(BF16) for v in grad_pre_coarse]
    coarse_grad[own, :] = mm(coarse_in[0], gpc[0], TN)
    coarse_grad[oth, :] = mm(coarse_in[1], gpc[0], TN)
    sent[3].start()
    grad_coarse_in = (
        mm(gpc[0], wc_own[own, :], NT) + mm(gpc[1], wc_oth[own, :], NT),
        mm(gpc[0], wc_own[oth, :], NT) + mm(gpc[1], wc_oth[oth, :], NT),
    )
    grad_one = tuple(g + mm(member, c.astype(BF16)) for g, c in zip(grad_two, grad_coarse_in))
    gpm = tuple(
        (g * (s + c * (1.0 - s))).astype(BF16) for g, s, c in zip(grad_one, sig_mesh, act_mesh)
    )
    process_grad[own, :] = mm(agg_own, gpm[0], TN)
    process_grad[oth, :] = mm(agg_oth, gpm[0], TN)
    sent[2].start()
    grad_agg = (mm(gpm[0], wp_own[own, :], NT) + mm(gpm[1], wp_oth[own, :], NT)).astype(BF16)
    grad_zero = (grad_one[0] + mm(reach, grad_agg, TN)).astype(BF16)
    for p in range(groups):
        span = slice(p * rows, (p + 1) * rows)
        grad_hidden = mm(cots[span, :], wd_own[...], NT) + mm(hit_t[span, :], grad_zero)
        gpe[span, :] = (grad_hidden * slope[span, :]).astype(BF16)
    encode_grad[...] = mm(cells[...], gpe[...], TN)
    sent[1].start()
    for copy in sent:
        copy.wait()


def replicated(
    fields,
    owner_group,
    owner_node,
    stencil_codes,
    coarse_ids,
    encode_weight,
    process_weight,
    coarse_weight,
    decode_weight,
    cotangent,
):
    mesh_count = lax.axis_size("mesh")
    tile_count = lax.axis_size("tile")
    groups = mesh_count * tile_count
    rows, c_in = fields.shape
    c_out = cotangent.shape[1]
    width = encode_weight.shape[1]
    nodes = groups * MA * MB
    block = rows + ID_ROWS
    weights = (encode_weight, process_weight, coarse_weight, decode_weight)
    swap = [(0, 1), (1, 0)]
    vmem = pl.BlockSpec(memory_space=pltpu.VMEM)
    hbm = pl.BlockSpec(memory_space=pl.ANY)
    payload = pl.pallas_call(
        pack_kernel,
        in_specs=[vmem] * 6,
        out_specs=vmem,
        out_shape=pltpu.VMEM((block, c_in), BF16),
        scratch_shapes=[pltpu.VMEM((ID_ROWS, rows), F32)],
    )(
        fields,
        owner_group.reshape(1, rows),
        owner_node.reshape(1, rows),
        stencil_codes.T,
        coarse_ids.reshape(1, MA * MB),
        cotangent,
    )
    payload, weights = lax.optimization_barrier((payload, weights))
    blocks = [payload]
    for shift in range(1, mesh_count):
        ring = [(i, (i + shift) % mesh_count) for i in range(mesh_count)]
        blocks.append(lax.ppermute(payload, "mesh", ring))
    others = tuple(lax.ppermute(w, "feat", swap) for w in weights)
    column = jnp.concatenate(blocks, axis=0)
    column, others = lax.optimization_barrier((column, others))
    columns = [column]
    for shift in range(1, tile_count):
        ring = [(i, (i + shift) % tile_count) for i in range(tile_count)]
        columns.append(lax.ppermute(column, "tile", ring))
    near = jnp.concatenate(columns, axis=0)
    far = lax.ppermute(near, "feat", swap)
    cells = groups * rows
    degree = stencil_codes.shape[1]
    tables = pl.pallas_call(
        functools.partial(index_kernel, mesh_count, tile_count, degree),
        in_specs=[vmem],
        out_specs=[vmem] * 4,
        out_shape=(
            pltpu.VMEM((nodes, cells), BF16),
            pltpu.VMEM((cells, nodes), BF16),
            pltpu.VMEM((nodes, nodes), BF16),
            pltpu.VMEM((nodes, CPD * groups), BF16),
        ),
        scratch_shapes=[pltpu.VMEM((nodes, ID_ROWS), F32)],
    )(held(near))
    outs = (
        jax.ShapeDtypeStruct((rows, c_out), F32),
        jax.ShapeDtypeStruct((c_in, width), F32),
        jax.ShapeDtypeStruct(process_weight.shape, F32),
        jax.ShapeDtypeStruct(coarse_weight.shape, F32),
        jax.ShapeDtypeStruct((width, c_out), F32),
    )
    return pl.pallas_call(
        functools.partial(step_kernel, groups),
        in_specs=[vmem] * 14,
        out_specs=[hbm] * 5,
        out_shape=outs,
        scratch_shapes=[
            pltpu.VMEM((cells, c_in), BF16),
            pltpu.VMEM((cells, c_out), BF16),
            pltpu.VMEM((cells, 2 * width), BF16),
            pltpu.VMEM((cells, width), F32),
            pltpu.VMEM((cells, width), BF16),
            *[pltpu.VMEM(o.shape, F32) for o in outs],
            pltpu.SemaphoreType.DMA((5,)),
        ],
    )(*map(held, (near, far, *tables, *weights, *others)))


def padded(array, sides, width):
    for axis, dim in sides:
        peers, length = (lax.axis_size(axis), array.shape[dim])
        up = [(i, (i + 1) % peers) for i in range(peers)]
        down = [(j, i) for i, j in up]
        last = lax.slice_in_dim(array, length - width, length, axis=dim)
        initial = lax.slice_in_dim(array, 0, width, axis=dim)
        before = lax.ppermute(last, axis, up)
        after = lax.ppermute(initial, axis, down)
        array = jnp.concatenate([before, array, after], axis=dim)
    return array


def silu_grad(pre):
    sig = jax.nn.sigmoid(pre)
    return sig * (1.0 + pre * (1.0 - sig))


def send_rows(outgoing, slot_node):
    feat_width = outgoing.shape[-1]
    got, got_node = (
        lax.all_to_all(outgoing, ("mesh", "tile"), split_axis=0, concat_axis=0, tiled=True),
        lax.all_to_all(slot_node, ("mesh", "tile"), split_axis=0, concat_axis=0, tiled=True),
    )
    return (got.reshape(-1, feat_width), got_node.reshape(-1))


def route_block(block, mesh_count, tile_count, purpose):
    feat_width = block.shape[-1]
    slot_count = block.shape[0] // (mesh_count * tile_count)
    flat_shape = (mesh_count * tile_count, slot_count, feat_width)
    if purpose == "reply":
        moved = lax.all_to_all(
            block.reshape(flat_shape), ("mesh", "tile"), split_axis=0, concat_axis=0, tiled=True
        )
    elif purpose == "gradient":
        moved = lax.all_to_all(
            block.reshape(flat_shape), ("mesh", "tile"), split_axis=0, concat_axis=0, tiled=True
        )
    else:
        moved = lax.all_to_all(
            block.reshape(flat_shape), ("mesh", "tile"), split_axis=0, concat_axis=0, tiled=True
        )
    return moved.reshape(-1, feat_width)


def distributed(
    fields,
    owner_group,
    owner_node,
    stencil_codes,
    coarse_ids,
    encode_weight,
    process_weight,
    coarse_weight,
    decode_weight,
    cotangent,
):
    highest = lax.Precision.HIGHEST
    row_count = fields.shape[0]
    mesh_count = lax.axis_size("mesh")
    tile_count = lax.axis_size("tile")
    groups = mesh_count * tile_count
    slot_count = 2 * row_count // groups
    feat_width = encode_weight.shape[1]
    patch_rows = MA
    patch_cols = MB
    nodes_local = patch_rows * patch_cols
    coarse_count = CPD * groups
    target = owner_group[:, 0]
    group_onehot = (target[:, None] == jnp.arange(groups, dtype=jnp.int32)[None, :]).astype(
        jnp.int32
    )
    earlier = jnp.cumsum(group_onehot, axis=0) - group_onehot
    position = target * slot_count + jnp.sum(earlier * group_onehot, axis=1)
    matches = jnp.arange(groups * slot_count, dtype=jnp.int32)[:, None] == position[None, :]
    dispatch = matches.astype(jnp.bfloat16)
    slot_node = (jnp.max(jnp.where(matches, owner_node[None, :] + 1, 0), axis=1) - 1).reshape(
        groups, slot_count
    )
    pre_encode = jnp.dot(fields, encode_weight, preferred_element_type=jnp.float32)
    hidden = jax.nn.silu(pre_encode).astype(jnp.bfloat16)
    outgoing = jnp.dot(dispatch, hidden, preferred_element_type=jnp.float32).astype(jnp.bfloat16)
    incoming, incoming_node = send_rows(outgoing.reshape(groups, slot_count, feat_width), slot_node)
    node_match = (
        incoming_node[:, None] == jnp.arange(nodes_local, dtype=jnp.int32)[None, :]
    ).astype(jnp.bfloat16)
    node_in = jnp.einsum(
        "sn,sh->nh", node_match, incoming, preferred_element_type=jnp.float32
    ).astype(jnp.bfloat16)
    counts = jnp.sum(
        (stencil_codes[:, :, None] == jnp.arange(25, dtype=jnp.int32)[None, None, :]).astype(
            jnp.float32
        ),
        axis=1,
    )
    counts = counts.astype(jnp.bfloat16).reshape(patch_rows, patch_cols, 25)
    padded_nodes, padded_counts = (
        padded(node_in.reshape(patch_rows, patch_cols, feat_width), (("mesh", 0), ("tile", 1)), 2),
        padded(counts, (("mesh", 0), ("tile", 1)), 2),
    )
    gathered = jnp.zeros((patch_rows, patch_cols, feat_width), jnp.float32)
    for code_index in range(25):
        step_x = code_index // 5 - 2
        step_y = code_index % 5 - 2
        weight_here = padded_counts[
            2 : 2 + patch_rows, 2 : 2 + patch_cols, code_index : code_index + 1
        ].astype(jnp.float32)
        gathered = gathered + weight_here * padded_nodes[
            2 + step_x : 2 + step_x + patch_rows, 2 + step_y : 2 + step_y + patch_cols
        ].astype(jnp.float32)
    agg = gathered.reshape(nodes_local, feat_width).astype(jnp.bfloat16)
    agg_full = lax.all_gather(agg, "feat", axis=1, tiled=True)
    pre_mesh = jnp.dot(agg_full, process_weight, preferred_element_type=jnp.float32)
    level_one = node_in.astype(jnp.float32) + jax.nn.silu(pre_mesh)
    coarse_match = (
        coarse_ids[:, None] == jnp.arange(coarse_count, dtype=jnp.int32)[None, :]
    ).astype(jnp.float32)
    coarse_part = jnp.dot(coarse_match.T, level_one, precision=highest)
    coarse_total = lax.psum(coarse_part, ("mesh", "tile"))
    coarse_in = lax.all_gather(coarse_total.astype(jnp.bfloat16), "feat", axis=1, tiled=True)
    pre_coarse = jnp.dot(coarse_in, coarse_weight, preferred_element_type=jnp.float32)
    coarse_out = jax.nn.silu(pre_coarse).astype(jnp.bfloat16)
    level_two = (
        level_one
        + jnp.dot(coarse_match.astype(jnp.bfloat16), coarse_out, preferred_element_type=jnp.float32)
    ).astype(jnp.bfloat16)
    reply_rows = jnp.dot(node_match, level_two, preferred_element_type=jnp.float32).astype(
        jnp.bfloat16
    )
    returned = route_block(reply_rows, mesh_count, tile_count, "reply")
    merged = (
        hidden.astype(jnp.float32)
        + jnp.einsum("sr,sh->rh", dispatch, returned, preferred_element_type=jnp.float32)
    ).astype(jnp.bfloat16)
    pred_part = jnp.dot(merged, decode_weight, preferred_element_type=jnp.float32)
    prediction = lax.psum(pred_part, "feat")
    decode_grad = jnp.dot(merged.astype(jnp.float32).T, cotangent, precision=highest)
    grad_merged = jnp.dot(cotangent, decode_weight.astype(jnp.float32).T, precision=highest)
    grad_out = jnp.dot(
        dispatch, grad_merged.astype(jnp.bfloat16), preferred_element_type=jnp.float32
    ).astype(jnp.bfloat16)
    grad_in = route_block(grad_out, mesh_count, tile_count, "gradient")
    grad_two = jnp.einsum("sn,sh->nh", node_match, grad_in, preferred_element_type=jnp.float32)
    coarse_grad_part = jnp.dot(coarse_match.T, grad_two, precision=highest)
    grad_coarse_out = lax.psum(coarse_grad_part, ("mesh", "tile"))
    grad_pre_coarse = grad_coarse_out * silu_grad(pre_coarse)
    coarse_grad = jnp.dot(coarse_in.astype(jnp.float32).T, grad_pre_coarse, precision=highest)
    grad_coarse_full = jnp.dot(
        grad_pre_coarse, coarse_weight.astype(jnp.float32).T, precision=highest
    )
    grad_coarse_in = lax.psum_scatter(grad_coarse_full, "feat", scatter_dimension=1, tiled=True)
    grad_one = grad_two + jnp.dot(coarse_match, grad_coarse_in, precision=highest)
    grad_pre_mesh = grad_one * silu_grad(pre_mesh)
    process_grad = jnp.dot(agg_full.astype(jnp.float32).T, grad_pre_mesh, precision=highest)
    grad_pre_full = lax.all_gather(grad_pre_mesh, "feat", axis=1, tiled=True)
    weight_full = lax.all_gather(process_weight, "feat", axis=1, tiled=True)
    own_rows = lax.dynamic_slice_in_dim(
        weight_full, lax.axis_index("feat") * feat_width, feat_width, 0
    )
    grad_agg = jnp.dot(grad_pre_full, own_rows.astype(jnp.float32).T, precision=highest).astype(
        jnp.bfloat16
    )
    padded_grad = padded(
        grad_agg.reshape(patch_rows, patch_cols, feat_width), (("mesh", 0), ("tile", 1)), 2
    )
    spread = jnp.zeros((patch_rows, patch_cols, feat_width), jnp.float32)
    for code_index in range(25):
        step_x = code_index // 5 - 2
        step_y = code_index % 5 - 2
        weight_there = padded_counts[
            2 - step_x : 2 - step_x + patch_rows,
            2 - step_y : 2 - step_y + patch_cols,
            code_index : code_index + 1,
        ].astype(jnp.float32)
        spread = spread + weight_there * padded_grad[
            2 - step_x : 2 - step_x + patch_rows, 2 - step_y : 2 - step_y + patch_cols
        ].astype(jnp.float32)
    grad_zero = (grad_one + spread.reshape(nodes_local, feat_width)).astype(jnp.bfloat16)
    back_rows = jnp.dot(node_match, grad_zero, preferred_element_type=jnp.float32).astype(
        jnp.bfloat16
    )
    grad_back = route_block(back_rows, mesh_count, tile_count, "return")
    grad_hidden = grad_merged + jnp.einsum(
        "sr,sh->rh", dispatch, grad_back, preferred_element_type=jnp.float32
    )
    grad_pre_encode = grad_hidden * silu_grad(pre_encode)
    encode_grad = jnp.dot(fields.astype(jnp.float32).T, grad_pre_encode, precision=highest)
    encode_grad, process_grad, decode_grad = lax.psum(
        (encode_grad, process_grad, decode_grad), ("mesh", "tile")
    )
    return (prediction, encode_grad, process_grad, coarse_grad, decode_grad)


def body(fields, owner_group, owner_node, stencil_codes, *rest):
    groups = lax.axis_size("mesh") * lax.axis_size("tile")
    rows, c_in = fields.shape
    cells, nodes = groups * rows, groups * MA * MB
    degree = stencil_codes.shape[1]
    fits = (
        cells * nodes <= REPLICATE_LIMIT
        and lax.axis_size("feat") == 2
        and rows == c_in == rest[-1].shape[1]
        and max(nodes, 25) <= 256
        and degree + 3 <= ID_ROWS
        and MA * MB <= rows
    )
    plan = replicated if fits else distributed
    return plan(fields, owner_group, owner_node, stencil_codes, *rest)


def solution(mesh):
    placed = (
        P(("parts", "mesh", "tile"), None),
        P(("mesh", "tile"), None),
        P(("mesh", "tile")),
        P(("mesh", "tile"), None),
        P(("mesh", "tile")),
        P(None, "feat"),
        P(None, "feat"),
        P(None, "feat"),
        P("feat", None),
        P(("parts", "mesh", "tile"), None),
    )
    return jax.shard_map(
        body,
        mesh=mesh,
        in_specs=placed,
        out_specs=(
            P(("parts", "mesh", "tile"), None),
            P("parts", "feat"),
            P("parts", "feat"),
            P("parts", "feat"),
            P(("parts", "feat"), None),
        ),
        check_vma=False,
    )
```

```python
import functools

import jax
import jax.numpy as jnp
from jax import lax
from jax.experimental import pallas as pl
from jax.experimental.pallas import tpu as pltpu
from jax.sharding import PartitionSpec as P


MA = 4
MB = 8
CPD = 2
ID_ROWS = 16
GRANT = 20 << 20
REPLICATE_LIMIT = 1 << 20

F32 = jnp.float32
BF16 = jnp.bfloat16
NN = (((1,), (0,)), ((), ()))
NT = (((1,), (1,)), ((), ()))
TN = (((0,), (0,)), ((), ()))


def mm(lhs, rhs, dims=NN):
    return lax.dot_general(lhs, rhs, dims, preferred_element_type=F32)


def split(value):
    high = value.astype(BF16)
    return high, (value - high.astype(F32)).astype(BF16)


def held(value):
    return pltpu.with_memory_space_constraint(value, pltpu.VMEM)


def pack_kernel(fields, group_row, node_row, codes, coarse_row, cotangent, out, wide):
    rows = fields.shape[0]
    degree, local = codes.shape
    core = lax.axis_index("feat")

    @pl.when(core == 0)
    def _():
        out[0:rows, :] = fields[...]

    @pl.when(core != 0)
    def _():
        out[0:rows, :] = cotangent[...].astype(BF16)

    wide[...] = jnp.zeros(wide.shape, F32)
    wide[0:1, :] = group_row[...].astype(F32)
    wide[1:2, :] = node_row[...].astype(F32)
    wide[2 : 2 + degree, 0:local] = codes[...].astype(F32)
    wide[2 + degree : 3 + degree, 0:local] = coarse_row[...].astype(F32)
    out[rows : rows + ID_ROWS, :] = wide[...].astype(BF16)


def tags_at(ref, start):
    tags = ref[pl.ds(start, ID_ROWS), :].astype(F32)
    return tags, jnp.transpose(tags)


def hits(tags, tags_t, nodes):
    local = MA * MB
    rows = tags.shape[1]
    sub = lax.broadcasted_iota(jnp.int32, (nodes, rows), 0).astype(F32)
    lane = lax.broadcasted_iota(jnp.int32, (rows, nodes), 1).astype(F32)
    by_node = (sub == tags[0:1, :] * local + tags[1:2, :]).astype(BF16)
    by_cell = (lane == tags_t[:, 0:1] * local + tags_t[:, 1:2]).astype(BF16)
    return by_node, by_cell


def near_kernel(
    groups,
    near,
    far,
    we_own,
    we_oth,
    node_part,
    cot_part,
    dec_part,
    hid_own,
    slope,
    hit_t,
    cells,
    cots,
    hit,
    hid,
):
    nodes = groups * MA * MB
    rows, width = hid_own.shape[0], we_own.shape[1]
    block = rows + ID_ROWS
    core = lax.axis_index("feat")
    for p in range(near.shape[0] // block):
        span = slice(p * rows, (p + 1) * rows)
        here = pl.ds(p * block, rows)
        hit[:, span], hit_t[span, :] = hits(*tags_at(near, p * block + rows), nodes)
        a, b = near[here, :], far[here, :]
        cell = jnp.where(core == 0, a, b)
        cells[span, :] = cell
        cots[span, :] = jnp.where(core == 0, b, a)
        pre = mm(cell, we_own[...])
        sig = jax.nn.sigmoid(pre)
        act = pre * sig
        hid[span, 0:width] = act.astype(BF16)
        slope[span, :] = sig + act * (1.0 - sig)
        pre = mm(cell, we_oth[...])
        hid[span, width:] = (pre * jax.nn.sigmoid(pre)).astype(BF16)
    cot = cots[...]
    hid_own[...] = hid[0:rows, :]
    node_part[...] = mm(hit[...], hid[...])
    cot_part[...] = mm(hit[...], cot)
    dec_part[...] = mm(hid[:, :width], cot, TN)


def index_kernel(
    mesh_count, tile_count, degree, near, rest, hit, reach_out, member_out, ids
):
    groups = mesh_count * tile_count
    local = MA * MB
    nodes = groups * local
    block = near.shape[0] // tile_count
    rows = block - ID_ROWS
    my_mesh = lax.axis_index("mesh")
    my_tile = lax.axis_index("tile")
    for p in range(groups):
        shift, turn = p // tile_count, p % tile_count
        group = lax.rem(my_mesh - shift + mesh_count, mesh_count) * tile_count + lax.rem(
            my_tile - turn + tile_count, tile_count
        )
        q = p - tile_count
        tags, tags_t = tags_at(near, p * block + rows) if q < 0 else tags_at(rest, q * block + rows)
        if q >= 0:
            span = slice(q * rows, (q + 1) * rows)
            hit[:, span] = hits(tags, tags_t, nodes)[0]
        ids[pl.ds(pl.multiple_of(group * local, local), local), :] = tags_t[0:local, :]

    tags = ids[...].astype(jnp.int32)
    index = lax.broadcasted_iota(jnp.int32, (nodes, ID_ROWS), 0)
    group, place = lax.div(index, local), lax.rem(index, local)
    row = lax.div(group, tile_count) * MA + lax.div(place, MB)
    col = lax.rem(group, tile_count) * MB + lax.rem(place, MB)
    tall, broad = mesh_count * MA, tile_count * MB
    row = lax.rem(row + lax.div(tags, 5) - 2 + tall, tall)
    col = lax.rem(col + lax.rem(tags, 5) - 2 + broad, broad)
    peer = (lax.div(row, MA) * tile_count + lax.div(col, MB)) * local
    peer = peer + lax.rem(row, MA) * MB + lax.rem(col, MB)
    over = lax.broadcasted_iota(jnp.int32, (nodes, nodes), 1)
    reach = jnp.zeros((nodes, nodes), F32)
    for k in range(2, 2 + degree):
        reach = reach + (over == peer[:, k : k + 1]).astype(F32)
    reach_out[...] = reach.astype(BF16)
    member_out[...] = (
        lax.broadcasted_iota(jnp.int32, (nodes, CPD * groups), 1)
        == tags[:, 2 + degree : 3 + degree]
    ).astype(BF16)


def step_kernel(
    near_count,
    rest,
    far,
    node_part,
    cot_part,
    dec_part,
    hid_own,
    slope_near,
    hit_t_near,
    cells_near,
    cots_near,
    hit,
    reach_ref,
    member_ref,
    we_own,
    wp_own,
    wc_own,
    wd_own,
    we_oth,
    wp_oth,
    wc_oth,
    wd_oth,
    prediction_out,
    encode_out,
    process_out,
    coarse_out,
    decode_out,
    cells,
    cots,
    hid,
    slope,
    gpe,
    gpe_near,
    hit_t,
    prediction,
    encode_grad,
    process_grad,
    coarse_grad,
    decode_grad,
    sems,
):
    rows, width = hid_own.shape[0], we_own.shape[1]
    block = rows + ID_ROWS
    count = rest.shape[0] // block
    core = lax.axis_index("feat")
    own = pl.ds(pl.multiple_of(core * width, width), width)
    oth = pl.ds(pl.multiple_of((1 - core) * width, width), width)
    sent = [
        pltpu.make_async_copy(source, target, sems.at[i])
        for i, (source, target) in enumerate(
            (
                (prediction, prediction_out),
                (encode_grad, encode_out),
                (process_grad, process_out),
                (coarse_grad, coarse_out),
                (decode_grad, decode_out),
            )
        )
    ]
    nodes = hit.shape[0]
    for p in range(count):
        here = pl.ds(p * block, rows)
        span = slice(p * rows, (p + 1) * rows)
        a, b = rest[here, :], far[here, :]
        cell = jnp.where(core == 0, a, b)
        cells[span, :] = cell
        cots[span, :] = jnp.where(core == 0, b, a)
        pre = mm(cell, we_own[...])
        sig = jax.nn.sigmoid(pre)
        act = pre * sig
        hid[span, 0:width] = act.astype(BF16)
        slope[span, :] = sig + act * (1.0 - sig)
        pre = mm(cell, we_oth[...])
        hid[span, width:] = (pre * jax.nn.sigmoid(pre)).astype(BF16)
        hit_t[span, :] = hits(*tags_at(rest, p * block + rows), nodes)[1]

    reach = reach_ref[...]
    member = member_ref[...]
    node_in = (node_part[...] + mm(hit[...], hid[...])).astype(BF16)
    agg = mm(reach, node_in).astype(BF16)
    agg_own, agg_oth = agg[:, :width], agg[:, width:]
    pre_mesh = (
        mm(agg_own, wp_own[own, :]) + mm(agg_oth, wp_own[oth, :]),
        mm(agg_own, wp_oth[own, :]) + mm(agg_oth, wp_oth[oth, :]),
    )
    sig_mesh = tuple(jax.nn.sigmoid(v) for v in pre_mesh)
    act_mesh = tuple(v * s for v, s in zip(pre_mesh, sig_mesh))
    level_one = (
        node_in[:, :width].astype(F32) + act_mesh[0],
        node_in[:, width:].astype(F32) + act_mesh[1],
    )
    coarse_in = []
    for v in level_one:
        high, low = split(v)
        coarse_in.append((mm(member, high, TN) + mm(member, low, TN)).astype(BF16))
    pre_coarse = (
        mm(coarse_in[0], wc_own[own, :]) + mm(coarse_in[1], wc_own[oth, :]),
        mm(coarse_in[0], wc_oth[own, :]) + mm(coarse_in[1], wc_oth[oth, :]),
    )
    sig_coarse = tuple(jax.nn.sigmoid(v) for v in pre_coarse)
    act_coarse = tuple(v * s for v, s in zip(pre_coarse, sig_coarse))
    level_two = tuple(
        (v + mm(member, c.astype(BF16))).astype(BF16) for v, c in zip(level_one, act_coarse)
    )
    mine = hit_t_near[0:rows, :]
    merged = (
        (hid_own[:, :width].astype(F32) + mm(mine, level_two[0])).astype(BF16),
        (hid_own[:, width:].astype(F32) + mm(mine, level_two[1])).astype(BF16),
    )
    prediction[...] = mm(merged[0], wd_own[...]) + mm(merged[1], wd_oth[...])

    cot = cots[...]
    node_cot = cot_part[...] + mm(hit[...], cot)
    cot_high, cot_low = split(node_cot)
    decode_grad[...] = (
        dec_part[...] + mm(hid[:, :width], cot, TN) + mm(level_two[0], cot_high, TN)
    )
    grad_two = tuple(mm(cot_high, w[...], NT) + mm(cot_low, w[...], NT) for w in (wd_own, wd_oth))
    gpc = []
    for g, s, c in zip(grad_two, sig_coarse, act_coarse):
        high, low = split(g)
        total = mm(member, high, TN) + mm(member, low, TN)
        gpc.append((total * (s + c * (1.0 - s))).astype(BF16))
    coarse_grad[own, :] = mm(coarse_in[0], gpc[0], TN)
    coarse_grad[oth, :] = mm(coarse_in[1], gpc[0], TN)

    @pl.when(core >= 0)
    def _():
        for i in (0, 3, 4):
            sent[i].start()

    grad_coarse_in = (
        mm(gpc[0], wc_own[own, :], NT) + mm(gpc[1], wc_oth[own, :], NT),
        mm(gpc[0], wc_own[oth, :], NT) + mm(gpc[1], wc_oth[oth, :], NT),
    )
    grad_one = tuple(g + mm(member, c.astype(BF16)) for g, c in zip(grad_two, grad_coarse_in))
    gpm = tuple(
        (g * (s + c * (1.0 - s))).astype(BF16) for g, s, c in zip(grad_one, sig_mesh, act_mesh)
    )
    process_grad[own, :] = mm(agg_own, gpm[0], TN)
    process_grad[oth, :] = mm(agg_oth, gpm[0], TN)

    @pl.when(core >= 0)
    def _():
        sent[2].start()

    grad_agg = (mm(gpm[0], wp_own[own, :], NT) + mm(gpm[1], wp_oth[own, :], NT)).astype(BF16)
    grad_zero = (grad_one[0] + mm(reach, grad_agg, TN)).astype(BF16)
    for p in range(count):
        span = slice(p * rows, (p + 1) * rows)
        grad_hidden = mm(cots[span, :], wd_own[...], NT) + mm(hit_t[span, :], grad_zero)
        gpe[span, :] = (grad_hidden * slope[span, :]).astype(BF16)
    for p in range(near_count):
        span = slice(p * rows, (p + 1) * rows)
        grad_hidden = mm(cots_near[span, :], wd_own[...], NT) + mm(hit_t_near[span, :], grad_zero)
        gpe_near[span, :] = (grad_hidden * slope_near[span, :]).astype(BF16)
    encode_grad[...] = mm(cells[...], gpe[...], TN) + mm(cells_near[...], gpe_near[...], TN)
    sent[1].start()
    for copy in sent:
        copy.wait()


def replicated(
    fields,
    owner_group,
    owner_node,
    stencil_codes,
    coarse_ids,
    encode_weight,
    process_weight,
    coarse_weight,
    decode_weight,
    cotangent,
):
    mesh_count = lax.axis_size("mesh")
    tile_count = lax.axis_size("tile")
    groups = mesh_count * tile_count
    rows, c_in = fields.shape
    c_out = cotangent.shape[1]
    width = encode_weight.shape[1]
    nodes = groups * MA * MB
    block = rows + ID_ROWS
    weights = (encode_weight, process_weight, coarse_weight, decode_weight)
    swap = [(0, 1), (1, 0)]
    vmem = pl.BlockSpec(memory_space=pltpu.VMEM)
    hbm = pl.BlockSpec(memory_space=pl.ANY)
    grant = pltpu.CompilerParams(vmem_limit_bytes=GRANT)
    payload = pl.pallas_call(
        pack_kernel,
        in_specs=[vmem] * 6,
        out_specs=vmem,
        out_shape=pltpu.VMEM((block, c_in), BF16),
        scratch_shapes=[pltpu.VMEM((ID_ROWS, rows), F32)],
    )(
        fields,
        owner_group.reshape(1, rows),
        owner_node.reshape(1, rows),
        stencil_codes.T,
        coarse_ids.reshape(1, MA * MB),
        cotangent,
    )
    columns = [payload]
    for turn in range(1, tile_count):
        ring = [(i, (i + turn) % tile_count) for i in range(tile_count)]
        columns.append(lax.ppermute(payload, "tile", ring))
    near = jnp.concatenate(columns, axis=0)
    near, weights = lax.optimization_barrier((near, weights))
    blocks = []
    for shift in range(1, mesh_count):
        ring = [(i, (i + shift) % mesh_count) for i in range(mesh_count)]
        blocks.append(lax.ppermute(near, "mesh", ring))
    near_far = lax.ppermute(near, "feat", swap)
    others = tuple(lax.ppermute(w, "feat", swap) for w in weights)
    degree = stencil_codes.shape[1]
    beside = tile_count * rows
    near_call = pl.pallas_call(
        functools.partial(near_kernel, groups),
        in_specs=[vmem] * 4,
        compiler_params=grant,
        out_specs=[vmem] * 8,
        out_shape=(
            pltpu.VMEM((nodes, 2 * width), F32),
            pltpu.VMEM((nodes, c_out), F32),
            pltpu.VMEM((width, c_out), F32),
            pltpu.VMEM((rows, 2 * width), BF16),
            pltpu.VMEM((beside, width), F32),
            pltpu.VMEM((beside, nodes), BF16),
            pltpu.VMEM((beside, c_in), BF16),
            pltpu.VMEM((beside, c_out), BF16),
        ),
        scratch_shapes=[
            pltpu.VMEM((nodes, beside), BF16),
            pltpu.VMEM((beside, 2 * width), BF16),
        ],
    )
    parts = near_call(*map(held, (near, near_far, encode_weight, others[0])))
    rest = jnp.concatenate(blocks, axis=0)
    rest_far = lax.ppermute(rest, "feat", swap)
    cells = (groups - tile_count) * rows
    tables = pl.pallas_call(
        functools.partial(index_kernel, mesh_count, tile_count, degree),
        in_specs=[vmem] * 2,
        compiler_params=grant,
        out_specs=[vmem] * 3,
        out_shape=(
            pltpu.VMEM((nodes, cells), BF16),
            pltpu.VMEM((nodes, nodes), BF16),
            pltpu.VMEM((nodes, CPD * groups), BF16),
        ),
        scratch_shapes=[pltpu.VMEM((nodes, ID_ROWS), F32)],
    )(held(near), held(rest))
    outs = (
        jax.ShapeDtypeStruct((rows, c_out), F32),
        jax.ShapeDtypeStruct((c_in, width), F32),
        jax.ShapeDtypeStruct(process_weight.shape, F32),
        jax.ShapeDtypeStruct(coarse_weight.shape, F32),
        jax.ShapeDtypeStruct((width, c_out), F32),
    )
    operands = [held(v) for v in (rest, rest_far, *parts, *tables, *weights, *others)]
    return pl.pallas_call(
        functools.partial(step_kernel, tile_count),
        in_specs=[vmem] * len(operands),
        compiler_params=grant,
        out_specs=[hbm] * 5,
        out_shape=outs,
        scratch_shapes=[
            pltpu.VMEM((cells, c_in), BF16),
            pltpu.VMEM((cells, c_out), BF16),
            pltpu.VMEM((cells, 2 * width), BF16),
            pltpu.VMEM((cells, width), F32),
            pltpu.VMEM((cells, width), BF16),
            pltpu.VMEM((beside, width), BF16),
            pltpu.VMEM((cells, nodes), BF16),
            *[pltpu.VMEM(o.shape, F32) for o in outs],
            pltpu.SemaphoreType.DMA((5,)),
        ],
    )(*operands)


def padded(array, sides, width):
    for axis, dim in sides:
        peers, length = (lax.axis_size(axis), array.shape[dim])
        up = [(i, (i + 1) % peers) for i in range(peers)]
        down = [(j, i) for i, j in up]
        last = lax.slice_in_dim(array, length - width, length, axis=dim)
        initial = lax.slice_in_dim(array, 0, width, axis=dim)
        before = lax.ppermute(last, axis, up)
        after = lax.ppermute(initial, axis, down)
        array = jnp.concatenate([before, array, after], axis=dim)
    return array


def silu_grad(pre):
    sig = jax.nn.sigmoid(pre)
    return sig * (1.0 + pre * (1.0 - sig))


def send_rows(outgoing, slot_node):
    feat_width = outgoing.shape[-1]
    got, got_node = (
        lax.all_to_all(outgoing, ("mesh", "tile"), split_axis=0, concat_axis=0, tiled=True),
        lax.all_to_all(slot_node, ("mesh", "tile"), split_axis=0, concat_axis=0, tiled=True),
    )
    return (got.reshape(-1, feat_width), got_node.reshape(-1))


def route_block(block, mesh_count, tile_count, purpose):
    feat_width = block.shape[-1]
    slot_count = block.shape[0] // (mesh_count * tile_count)
    flat_shape = (mesh_count * tile_count, slot_count, feat_width)
    if purpose == "reply":
        moved = lax.all_to_all(
            block.reshape(flat_shape), ("mesh", "tile"), split_axis=0, concat_axis=0, tiled=True
        )
    elif purpose == "gradient":
        moved = lax.all_to_all(
            block.reshape(flat_shape), ("mesh", "tile"), split_axis=0, concat_axis=0, tiled=True
        )
    else:
        moved = lax.all_to_all(
            block.reshape(flat_shape), ("mesh", "tile"), split_axis=0, concat_axis=0, tiled=True
        )
    return moved.reshape(-1, feat_width)


def distributed(
    fields,
    owner_group,
    owner_node,
    stencil_codes,
    coarse_ids,
    encode_weight,
    process_weight,
    coarse_weight,
    decode_weight,
    cotangent,
):
    highest = lax.Precision.HIGHEST
    row_count = fields.shape[0]
    mesh_count = lax.axis_size("mesh")
    tile_count = lax.axis_size("tile")
    groups = mesh_count * tile_count
    slot_count = 2 * row_count // groups
    feat_width = encode_weight.shape[1]
    patch_rows = MA
    patch_cols = MB
    nodes_local = patch_rows * patch_cols
    coarse_count = CPD * groups
    target = owner_group[:, 0]
    group_onehot = (target[:, None] == jnp.arange(groups, dtype=jnp.int32)[None, :]).astype(
        jnp.int32
    )
    earlier = jnp.cumsum(group_onehot, axis=0) - group_onehot
    position = target * slot_count + jnp.sum(earlier * group_onehot, axis=1)
    matches = jnp.arange(groups * slot_count, dtype=jnp.int32)[:, None] == position[None, :]
    dispatch = matches.astype(jnp.bfloat16)
    slot_node = (jnp.max(jnp.where(matches, owner_node[None, :] + 1, 0), axis=1) - 1).reshape(
        groups, slot_count
    )
    pre_encode = jnp.dot(fields, encode_weight, preferred_element_type=jnp.float32)
    hidden = jax.nn.silu(pre_encode).astype(jnp.bfloat16)
    outgoing = jnp.dot(dispatch, hidden, preferred_element_type=jnp.float32).astype(jnp.bfloat16)
    incoming, incoming_node = send_rows(outgoing.reshape(groups, slot_count, feat_width), slot_node)
    node_match = (
        incoming_node[:, None] == jnp.arange(nodes_local, dtype=jnp.int32)[None, :]
    ).astype(jnp.bfloat16)
    node_in = jnp.einsum(
        "sn,sh->nh", node_match, incoming, preferred_element_type=jnp.float32
    ).astype(jnp.bfloat16)
    counts = jnp.sum(
        (stencil_codes[:, :, None] == jnp.arange(25, dtype=jnp.int32)[None, None, :]).astype(
            jnp.float32
        ),
        axis=1,
    )
    counts = counts.astype(jnp.bfloat16).reshape(patch_rows, patch_cols, 25)
    padded_nodes, padded_counts = (
        padded(node_in.reshape(patch_rows, patch_cols, feat_width), (("mesh", 0), ("tile", 1)), 2),
        padded(counts, (("mesh", 0), ("tile", 1)), 2),
    )
    gathered = jnp.zeros((patch_rows, patch_cols, feat_width), jnp.float32)
    for code_index in range(25):
        step_x = code_index // 5 - 2
        step_y = code_index % 5 - 2
        weight_here = padded_counts[
            2 : 2 + patch_rows, 2 : 2 + patch_cols, code_index : code_index + 1
        ].astype(jnp.float32)
        gathered = gathered + weight_here * padded_nodes[
            2 + step_x : 2 + step_x + patch_rows, 2 + step_y : 2 + step_y + patch_cols
        ].astype(jnp.float32)
    agg = gathered.reshape(nodes_local, feat_width).astype(jnp.bfloat16)
    agg_full = lax.all_gather(agg, "feat", axis=1, tiled=True)
    pre_mesh = jnp.dot(agg_full, process_weight, preferred_element_type=jnp.float32)
    level_one = node_in.astype(jnp.float32) + jax.nn.silu(pre_mesh)
    coarse_match = (
        coarse_ids[:, None] == jnp.arange(coarse_count, dtype=jnp.int32)[None, :]
    ).astype(jnp.float32)
    coarse_part = jnp.dot(coarse_match.T, level_one, precision=highest)
    coarse_total = lax.psum(coarse_part, ("mesh", "tile"))
    coarse_in = lax.all_gather(coarse_total.astype(jnp.bfloat16), "feat", axis=1, tiled=True)
    pre_coarse = jnp.dot(coarse_in, coarse_weight, preferred_element_type=jnp.float32)
    coarse_out = jax.nn.silu(pre_coarse).astype(jnp.bfloat16)
    level_two = (
        level_one
        + jnp.dot(coarse_match.astype(jnp.bfloat16), coarse_out, preferred_element_type=jnp.float32)
    ).astype(jnp.bfloat16)
    reply_rows = jnp.dot(node_match, level_two, preferred_element_type=jnp.float32).astype(
        jnp.bfloat16
    )
    returned = route_block(reply_rows, mesh_count, tile_count, "reply")
    merged = (
        hidden.astype(jnp.float32)
        + jnp.einsum("sr,sh->rh", dispatch, returned, preferred_element_type=jnp.float32)
    ).astype(jnp.bfloat16)
    pred_part = jnp.dot(merged, decode_weight, preferred_element_type=jnp.float32)
    prediction = lax.psum(pred_part, "feat")
    decode_grad = jnp.dot(merged.astype(jnp.float32).T, cotangent, precision=highest)
    grad_merged = jnp.dot(cotangent, decode_weight.astype(jnp.float32).T, precision=highest)
    grad_out = jnp.dot(
        dispatch, grad_merged.astype(jnp.bfloat16), preferred_element_type=jnp.float32
    ).astype(jnp.bfloat16)
    grad_in = route_block(grad_out, mesh_count, tile_count, "gradient")
    grad_two = jnp.einsum("sn,sh->nh", node_match, grad_in, preferred_element_type=jnp.float32)
    coarse_grad_part = jnp.dot(coarse_match.T, grad_two, precision=highest)
    grad_coarse_out = lax.psum(coarse_grad_part, ("mesh", "tile"))
    grad_pre_coarse = grad_coarse_out * silu_grad(pre_coarse)
    coarse_grad = jnp.dot(coarse_in.astype(jnp.float32).T, grad_pre_coarse, precision=highest)
    grad_coarse_full = jnp.dot(
        grad_pre_coarse, coarse_weight.astype(jnp.float32).T, precision=highest
    )
    grad_coarse_in = lax.psum_scatter(grad_coarse_full, "feat", scatter_dimension=1, tiled=True)
    grad_one = grad_two + jnp.dot(coarse_match, grad_coarse_in, precision=highest)
    grad_pre_mesh = grad_one * silu_grad(pre_mesh)
    process_grad = jnp.dot(agg_full.astype(jnp.float32).T, grad_pre_mesh, precision=highest)
    grad_pre_full = lax.all_gather(grad_pre_mesh, "feat", axis=1, tiled=True)
    weight_full = lax.all_gather(process_weight, "feat", axis=1, tiled=True)
    own_rows = lax.dynamic_slice_in_dim(
        weight_full, lax.axis_index("feat") * feat_width, feat_width, 0
    )
    grad_agg = jnp.dot(grad_pre_full, own_rows.astype(jnp.float32).T, precision=highest).astype(
        jnp.bfloat16
    )
    padded_grad = padded(
        grad_agg.reshape(patch_rows, patch_cols, feat_width), (("mesh", 0), ("tile", 1)), 2
    )
    spread = jnp.zeros((patch_rows, patch_cols, feat_width), jnp.float32)
    for code_index in range(25):
        step_x = code_index // 5 - 2
        step_y = code_index % 5 - 2
        weight_there = padded_counts[
            2 - step_x : 2 - step_x + patch_rows,
            2 - step_y : 2 - step_y + patch_cols,
            code_index : code_index + 1,
        ].astype(jnp.float32)
        spread = spread + weight_there * padded_grad[
            2 - step_x : 2 - step_x + patch_rows, 2 - step_y : 2 - step_y + patch_cols
        ].astype(jnp.float32)
    grad_zero = (grad_one + spread.reshape(nodes_local, feat_width)).astype(jnp.bfloat16)
    back_rows = jnp.dot(node_match, grad_zero, preferred_element_type=jnp.float32).astype(
        jnp.bfloat16
    )
    grad_back = route_block(back_rows, mesh_count, tile_count, "return")
    grad_hidden = grad_merged + jnp.einsum(
        "sr,sh->rh", dispatch, grad_back, preferred_element_type=jnp.float32
    )
    grad_pre_encode = grad_hidden * silu_grad(pre_encode)
    encode_grad = jnp.dot(fields.astype(jnp.float32).T, grad_pre_encode, precision=highest)
    encode_grad, process_grad, decode_grad = lax.psum(
        (encode_grad, process_grad, decode_grad), ("mesh", "tile")
    )
    return (prediction, encode_grad, process_grad, coarse_grad, decode_grad)


def body(fields, owner_group, owner_node, stencil_codes, *rest):
    groups = lax.axis_size("mesh") * lax.axis_size("tile")
    rows, c_in = fields.shape
    cells, nodes = groups * rows, groups * MA * MB
    degree = stencil_codes.shape[1]
    fits = (
        groups > lax.axis_size("tile")
        and cells * nodes <= REPLICATE_LIMIT
        and lax.axis_size("feat") == 2
        and rows == c_in == rest[-1].shape[1]
        and max(nodes, 25) <= 256
        and degree + 3 <= ID_ROWS
        and MA * MB <= rows
    )
    plan = replicated if fits else distributed
    return plan(fields, owner_group, owner_node, stencil_codes, *rest)


def solution(mesh):
    placed = (
        P(("parts", "mesh", "tile"), None),
        P(("mesh", "tile"), None),
        P(("mesh", "tile")),
        P(("mesh", "tile"), None),
        P(("mesh", "tile")),
        P(None, "feat"),
        P(None, "feat"),
        P(None, "feat"),
        P("feat", None),
        P(("parts", "mesh", "tile"), None),
    )
    return jax.shard_map(
        body,
        mesh=mesh,
        in_specs=placed,
        out_specs=(
            P(("parts", "mesh", "tile"), None),
            P("parts", "feat"),
            P("parts", "feat"),
            P("parts", "feat"),
            P(("parts", "feat"), None),
        ),
        check_vma=False,
    )
```

```python
import functools

import jax
import jax.numpy as jnp
from jax import lax
from jax.experimental import pallas as pl
from jax.experimental.pallas import tpu as pltpu
from jax.sharding import PartitionSpec as P


MA = 4
MB = 8
CPD = 2
ID_ROWS = 16
EARLY = 3
GRANT = 20 << 20
REPLICATE_LIMIT = 1 << 20

F32 = jnp.float32
BF16 = jnp.bfloat16
NN = (((1,), (0,)), ((), ()))
NT = (((1,), (1,)), ((), ()))
TN = (((0,), (0,)), ((), ()))


def mm(lhs, rhs, dims=NN):
    return lax.dot_general(lhs, rhs, dims, preferred_element_type=F32)


def split(value):
    high = value.astype(BF16)
    return high, (value - high.astype(F32)).astype(BF16)


def held(value):
    return pltpu.with_memory_space_constraint(value, pltpu.VMEM)


def pack_kernel(fields, group_row, node_row, codes, coarse_row, cotangent, out, wide):
    rows = fields.shape[0]
    degree, local = codes.shape
    core = lax.axis_index("feat")

    @pl.when(core == 0)
    def _():
        out[0:rows, :] = fields[...]

    @pl.when(core != 0)
    def _():
        out[0:rows, :] = cotangent[...].astype(BF16)

    wide[...] = jnp.zeros(wide.shape, F32)
    wide[0:1, :] = group_row[...].astype(F32)
    wide[1:2, :] = node_row[...].astype(F32)
    wide[2 : 2 + degree, 0:local] = codes[...].astype(F32)
    wide[2 + degree : 3 + degree, 0:local] = coarse_row[...].astype(F32)
    out[rows : rows + ID_ROWS, :] = wide[...].astype(BF16)


def tags_at(ref, start):
    tags = ref[pl.ds(start, ID_ROWS), :].astype(F32)
    return tags, jnp.transpose(tags)


def hits(tags, tags_t, nodes):
    local = MA * MB
    rows = tags.shape[1]
    sub = lax.broadcasted_iota(jnp.int32, (nodes, rows), 0).astype(F32)
    lane = lax.broadcasted_iota(jnp.int32, (rows, nodes), 1).astype(F32)
    by_node = (sub == tags[0:1, :] * local + tags[1:2, :]).astype(BF16)
    by_cell = (lane == tags_t[:, 0:1] * local + tags_t[:, 1:2]).astype(BF16)
    return by_node, by_cell


def near_kernel(
    groups,
    near,
    far,
    we_own,
    we_oth,
    wd_own,
    node_part,
    cot_part,
    dec_part,
    hid_own,
    slope,
    hit_t,
    cells,
    gm,
    hit,
    cots,
    hid,
):
    nodes = groups * MA * MB
    rows, width = hid_own.shape[0], we_own.shape[1]
    block = rows + ID_ROWS
    core = lax.axis_index("feat")
    for p in range(near.shape[0] // block):
        span = slice(p * rows, (p + 1) * rows)
        here = pl.ds(p * block, rows)
        hit[:, span], hit_t[span, :] = hits(*tags_at(near, p * block + rows), nodes)
        a, b = near[here, :], far[here, :]
        cell = jnp.where(core == 0, a, b)
        cells[span, :] = cell
        cots[span, :] = jnp.where(core == 0, b, a)
        pre = mm(cell, we_own[...])
        sig = jax.nn.sigmoid(pre)
        act = pre * sig
        hid[span, 0:width] = act.astype(BF16)
        slope[span, :] = sig + act * (1.0 - sig)
        pre = mm(cell, we_oth[...])
        hid[span, width:] = (pre * jax.nn.sigmoid(pre)).astype(BF16)
    cot = cots[...]
    hid_own[...] = hid[0:rows, :]
    node_part[...] = mm(hit[...], hid[...])
    cot_part[...] = mm(hit[...], cot)
    dec_part[...] = mm(hid[:, :width], cot, TN)
    gm[...] = mm(cot, wd_own[...], NT)


def index_kernel(
    shifts, tile_count, degree, near, rest, hit, hit_t, reach_out, member_out, ids
):
    mesh_count = len(shifts)
    groups = mesh_count * tile_count
    local = MA * MB
    nodes = groups * local
    block = (near.shape[0] + rest.shape[0]) // groups
    count = near.shape[0] // block
    rows = block - ID_ROWS
    my_mesh = lax.axis_index("mesh")
    my_tile = lax.axis_index("tile")
    for p in range(groups):
        shift, turn = shifts[p // tile_count], p % tile_count
        group = lax.rem(my_mesh - shift + mesh_count, mesh_count) * tile_count + lax.rem(
            my_tile - turn + tile_count, tile_count
        )
        q = p - count
        tags, tags_t = tags_at(near, p * block + rows) if q < 0 else tags_at(rest, q * block + rows)
        if q >= 0:
            span = slice(q * rows, (q + 1) * rows)
            hit[:, span], hit_t[span, :] = hits(tags, tags_t, nodes)
        ids[pl.ds(pl.multiple_of(group * local, local), local), :] = tags_t[0:local, :]

    tags = ids[...].astype(jnp.int32)
    index = lax.broadcasted_iota(jnp.int32, (nodes, ID_ROWS), 0)
    group, place = lax.div(index, local), lax.rem(index, local)
    row = lax.div(group, tile_count) * MA + lax.div(place, MB)
    col = lax.rem(group, tile_count) * MB + lax.rem(place, MB)
    tall, broad = mesh_count * MA, tile_count * MB
    row = lax.rem(row + lax.div(tags, 5) - 2 + tall, tall)
    col = lax.rem(col + lax.rem(tags, 5) - 2 + broad, broad)
    peer = (lax.div(row, MA) * tile_count + lax.div(col, MB)) * local
    peer = peer + lax.rem(row, MA) * MB + lax.rem(col, MB)
    over = lax.broadcasted_iota(jnp.int32, (nodes, nodes), 1)
    reach = jnp.zeros((nodes, nodes), F32)
    for k in range(2, 2 + degree):
        reach = reach + (over == peer[:, k : k + 1]).astype(F32)
    reach_out[...] = reach.astype(BF16)
    member_out[...] = (
        lax.broadcasted_iota(jnp.int32, (nodes, CPD * groups), 1)
        == tags[:, 2 + degree : 3 + degree]
    ).astype(BF16)


def step_kernel(
    near_count,
    rest,
    far,
    node_part,
    cot_part,
    dec_part,
    hid_own,
    slope_near,
    hit_t_near,
    cells_near,
    gm_near,
    hit,
    hit_t,
    reach_ref,
    member_ref,
    we_own,
    wp_own,
    wc_own,
    wd_own,
    we_oth,
    wp_oth,
    wc_oth,
    wd_oth,
    prediction_out,
    encode_out,
    process_out,
    coarse_out,
    decode_out,
    cells,
    cots,
    hid,
    slope,
    gpe,
    gpe_near,
    gm,
    prediction,
    encode_grad,
    process_grad,
    coarse_grad,
    decode_grad,
    sems,
):
    rows, width = hid_own.shape[0], we_own.shape[1]
    block = rows + ID_ROWS
    count = rest.shape[0] // block
    core = lax.axis_index("feat")
    own = pl.ds(pl.multiple_of(core * width, width), width)
    oth = pl.ds(pl.multiple_of((1 - core) * width, width), width)
    pairs = (
        (prediction, prediction_out),
        (encode_grad, encode_out),
        (process_grad, process_out),
        (coarse_grad, coarse_out),
        (decode_grad, decode_out),
    )

    def half_copy(i, half):
        source, target = pairs[i]
        size = source.shape[0] // 2
        part = pl.ds(pl.multiple_of(half * size, size), size)
        return pltpu.make_async_copy(source.at[part], target.at[part], sems.at[i, half])

    def launch(*chosen):
        def start(half, carry):
            for i in chosen:
                half_copy(i, half).start()
            return carry

        lax.fori_loop(0, 2, start, 0)

    for p in range(count):
        here = pl.ds(p * block, rows)
        span = slice(p * rows, (p + 1) * rows)
        a, b = rest[here, :], far[here, :]
        cell = jnp.where(core == 0, a, b)
        cells[span, :] = cell
        cots[span, :] = jnp.where(core == 0, b, a)
        pre = mm(cell, we_own[...])
        sig = jax.nn.sigmoid(pre)
        act = pre * sig
        hid[span, 0:width] = act.astype(BF16)
        slope[span, :] = sig + act * (1.0 - sig)
        pre = mm(cell, we_oth[...])
        hid[span, width:] = (pre * jax.nn.sigmoid(pre)).astype(BF16)

    reach = reach_ref[...]
    member = member_ref[...]
    node_in = (node_part[...] + mm(hit[...], hid[...])).astype(BF16)
    agg = mm(reach, node_in).astype(BF16)
    agg_own, agg_oth = agg[:, :width], agg[:, width:]
    pre_mesh = (
        mm(agg_own, wp_own[own, :]) + mm(agg_oth, wp_own[oth, :]),
        mm(agg_own, wp_oth[own, :]) + mm(agg_oth, wp_oth[oth, :]),
    )
    sig_mesh = tuple(jax.nn.sigmoid(v) for v in pre_mesh)
    act_mesh = tuple(v * s for v, s in zip(pre_mesh, sig_mesh))
    level_one = (
        node_in[:, :width].astype(F32) + act_mesh[0],
        node_in[:, width:].astype(F32) + act_mesh[1],
    )
    coarse_in = []
    for v in level_one:
        high, low = split(v)
        coarse_in.append((mm(member, high, TN) + mm(member, low, TN)).astype(BF16))
    pre_coarse = (
        mm(coarse_in[0], wc_own[own, :]) + mm(coarse_in[1], wc_own[oth, :]),
        mm(coarse_in[0], wc_oth[own, :]) + mm(coarse_in[1], wc_oth[oth, :]),
    )
    sig_coarse = tuple(jax.nn.sigmoid(v) for v in pre_coarse)
    act_coarse = tuple(v * s for v, s in zip(pre_coarse, sig_coarse))
    level_two = tuple(
        (v + mm(member, c.astype(BF16))).astype(BF16) for v, c in zip(level_one, act_coarse)
    )
    mine = hit_t_near[0:rows, :]
    merged = (
        (hid_own[:, :width].astype(F32) + mm(mine, level_two[0])).astype(BF16),
        (hid_own[:, width:].astype(F32) + mm(mine, level_two[1])).astype(BF16),
    )
    prediction[...] = mm(merged[0], wd_own[...]) + mm(merged[1], wd_oth[...])

    cot = cots[...]
    gm[...] = mm(cot, wd_own[...], NT)
    node_cot = cot_part[...] + mm(hit[...], cot)
    cot_high, cot_low = split(node_cot)
    decode_grad[...] = (
        dec_part[...] + mm(hid[:, :width], cot, TN) + mm(level_two[0], cot_high, TN)
    )
    grad_two = tuple(mm(cot_high, w[...], NT) + mm(cot_low, w[...], NT) for w in (wd_own, wd_oth))
    gpc = []
    for g, s, c in zip(grad_two, sig_coarse, act_coarse):
        high, low = split(g)
        total = mm(member, high, TN) + mm(member, low, TN)
        gpc.append((total * (s + c * (1.0 - s))).astype(BF16))
    coarse_grad[own, :] = mm(coarse_in[0], gpc[0], TN)
    coarse_grad[oth, :] = mm(coarse_in[1], gpc[0], TN)


    grad_coarse_in = (
        mm(gpc[0], wc_own[own, :], NT) + mm(gpc[1], wc_oth[own, :], NT),
        mm(gpc[0], wc_own[oth, :], NT) + mm(gpc[1], wc_oth[oth, :], NT),
    )
    grad_one = tuple(g + mm(member, c.astype(BF16)) for g, c in zip(grad_two, grad_coarse_in))
    gpm = tuple(
        (g * (s + c * (1.0 - s))).astype(BF16) for g, s, c in zip(grad_one, sig_mesh, act_mesh)
    )
    process_grad[own, :] = mm(agg_own, gpm[0], TN)
    process_grad[oth, :] = mm(agg_oth, gpm[0], TN)

    launch(0, 2, 3, 4)

    grad_agg = (mm(gpm[0], wp_own[own, :], NT) + mm(gpm[1], wp_oth[own, :], NT)).astype(BF16)
    grad_zero = (grad_one[0] + mm(reach, grad_agg, TN)).astype(BF16)
    for p in range(count):
        span = slice(p * rows, (p + 1) * rows)
        grad_hidden = gm[span, :] + mm(hit_t[span, :], grad_zero)
        gpe[span, :] = (grad_hidden * slope[span, :]).astype(BF16)
    for p in range(near_count):
        span = slice(p * rows, (p + 1) * rows)
        grad_hidden = gm_near[span, :] + mm(hit_t_near[span, :], grad_zero)
        gpe_near[span, :] = (grad_hidden * slope_near[span, :]).astype(BF16)
    encode_grad[...] = mm(cells[...], gpe[...], TN) + mm(cells_near[...], gpe_near[...], TN)
    launch(1)
    for i in range(len(pairs)):
        for half in range(2):
            half_copy(i, half).wait()


def replicated(
    fields,
    owner_group,
    owner_node,
    stencil_codes,
    coarse_ids,
    encode_weight,
    process_weight,
    coarse_weight,
    decode_weight,
    cotangent,
):
    mesh_count = lax.axis_size("mesh")
    tile_count = lax.axis_size("tile")
    groups = mesh_count * tile_count
    rows, c_in = fields.shape
    c_out = cotangent.shape[1]
    width = encode_weight.shape[1]
    nodes = groups * MA * MB
    block = rows + ID_ROWS
    weights = (encode_weight, process_weight, coarse_weight, decode_weight)
    swap = [(0, 1), (1, 0)]
    vmem = pl.BlockSpec(memory_space=pltpu.VMEM)
    hbm = pl.BlockSpec(memory_space=pl.ANY)
    grant = pltpu.CompilerParams(vmem_limit_bytes=GRANT)
    payload = pl.pallas_call(
        pack_kernel,
        in_specs=[vmem] * 6,
        out_specs=vmem,
        out_shape=pltpu.VMEM((block, c_in), BF16),
        scratch_shapes=[pltpu.VMEM((ID_ROWS, rows), F32)],
    )(
        fields,
        owner_group.reshape(1, rows),
        owner_node.reshape(1, rows),
        stencil_codes.T,
        coarse_ids.reshape(1, MA * MB),
        cotangent,
    )
    columns = [payload]
    for turn in range(1, tile_count):
        ring = [(i, (i + turn) % tile_count) for i in range(tile_count)]
        columns.append(lax.ppermute(payload, "tile", ring))
    near = jnp.concatenate(columns, axis=0)
    near, weights = lax.optimization_barrier((near, weights))
    shifts = [0, EARLY, *[i for i in range(1, mesh_count) if i != EARLY]]
    blocks = [near]
    for shift in shifts[1:]:
        ring = [(i, (i + shift) % mesh_count) for i in range(mesh_count)]
        blocks.append(lax.ppermute(near, "mesh", ring))
    near_far = lax.ppermute(near, "feat", swap)
    others = tuple(lax.ppermute(w, "feat", swap) for w in weights)
    early_far = lax.ppermute(blocks[1], "feat", swap)
    near = jnp.concatenate(blocks[:2], axis=0)
    near_far = jnp.concatenate([near_far, early_far], axis=0)
    degree = stencil_codes.shape[1]
    beside = 2 * tile_count * rows
    near_call = pl.pallas_call(
        functools.partial(near_kernel, groups),
        in_specs=[vmem] * 5,
        compiler_params=grant,
        out_specs=[vmem] * 8,
        out_shape=(
            pltpu.VMEM((nodes, 2 * width), F32),
            pltpu.VMEM((nodes, c_out), F32),
            pltpu.VMEM((width, c_out), F32),
            pltpu.VMEM((rows, 2 * width), BF16),
            pltpu.VMEM((beside, width), F32),
            pltpu.VMEM((beside, nodes), BF16),
            pltpu.VMEM((beside, c_in), BF16),
            pltpu.VMEM((beside, width), F32),
        ),
        scratch_shapes=[
            pltpu.VMEM((nodes, beside), BF16),
            pltpu.VMEM((beside, c_out), BF16),
            pltpu.VMEM((beside, 2 * width), BF16),
        ],
    )
    parts = near_call(*map(held, (near, near_far, encode_weight, others[0], decode_weight)))
    rest = jnp.concatenate(blocks[2:], axis=0)
    rest_far = lax.ppermute(rest, "feat", swap)
    cells = (groups - 2 * tile_count) * rows
    tables = pl.pallas_call(
        functools.partial(index_kernel, shifts, tile_count, degree),
        in_specs=[vmem] * 2,
        compiler_params=grant,
        out_specs=[vmem] * 4,
        out_shape=(
            pltpu.VMEM((nodes, cells), BF16),
            pltpu.VMEM((cells, nodes), BF16),
            pltpu.VMEM((nodes, nodes), BF16),
            pltpu.VMEM((nodes, CPD * groups), BF16),
        ),
        scratch_shapes=[pltpu.VMEM((nodes, ID_ROWS), F32)],
    )(held(near), held(rest))
    outs = (
        jax.ShapeDtypeStruct((rows, c_out), F32),
        jax.ShapeDtypeStruct((c_in, width), F32),
        jax.ShapeDtypeStruct(process_weight.shape, F32),
        jax.ShapeDtypeStruct(coarse_weight.shape, F32),
        jax.ShapeDtypeStruct((width, c_out), F32),
    )
    operands = [held(v) for v in (rest, rest_far, *parts, *tables, *weights, *others)]
    return pl.pallas_call(
        functools.partial(step_kernel, 2 * tile_count),
        in_specs=[vmem] * len(operands),
        compiler_params=grant,
        out_specs=[hbm] * 5,
        out_shape=outs,
        scratch_shapes=[
            pltpu.VMEM((cells, c_in), BF16),
            pltpu.VMEM((cells, c_out), BF16),
            pltpu.VMEM((cells, 2 * width), BF16),
            pltpu.VMEM((cells, width), F32),
            pltpu.VMEM((cells, width), BF16),
            pltpu.VMEM((beside, width), BF16),
            pltpu.VMEM((cells, width), F32),
            *[pltpu.VMEM(o.shape, F32) for o in outs],
            pltpu.SemaphoreType.DMA((5, 2)),
        ],
    )(*operands)


def padded(array, sides, width):
    for axis, dim in sides:
        peers, length = (lax.axis_size(axis), array.shape[dim])
        up = [(i, (i + 1) % peers) for i in range(peers)]
        down = [(j, i) for i, j in up]
        last = lax.slice_in_dim(array, length - width, length, axis=dim)
        initial = lax.slice_in_dim(array, 0, width, axis=dim)
        before = lax.ppermute(last, axis, up)
        after = lax.ppermute(initial, axis, down)
        array = jnp.concatenate([before, array, after], axis=dim)
    return array


def silu_grad(pre):
    sig = jax.nn.sigmoid(pre)
    return sig * (1.0 + pre * (1.0 - sig))


def send_rows(outgoing, slot_node):
    feat_width = outgoing.shape[-1]
    got, got_node = (
        lax.all_to_all(outgoing, ("mesh", "tile"), split_axis=0, concat_axis=0, tiled=True),
        lax.all_to_all(slot_node, ("mesh", "tile"), split_axis=0, concat_axis=0, tiled=True),
    )
    return (got.reshape(-1, feat_width), got_node.reshape(-1))


def route_block(block, mesh_count, tile_count, purpose):
    feat_width = block.shape[-1]
    slot_count = block.shape[0] // (mesh_count * tile_count)
    flat_shape = (mesh_count * tile_count, slot_count, feat_width)
    if purpose == "reply":
        moved = lax.all_to_all(
            block.reshape(flat_shape), ("mesh", "tile"), split_axis=0, concat_axis=0, tiled=True
        )
    elif purpose == "gradient":
        moved = lax.all_to_all(
            block.reshape(flat_shape), ("mesh", "tile"), split_axis=0, concat_axis=0, tiled=True
        )
    else:
        moved = lax.all_to_all(
            block.reshape(flat_shape), ("mesh", "tile"), split_axis=0, concat_axis=0, tiled=True
        )
    return moved.reshape(-1, feat_width)


def distributed(
    fields,
    owner_group,
    owner_node,
    stencil_codes,
    coarse_ids,
    encode_weight,
    process_weight,
    coarse_weight,
    decode_weight,
    cotangent,
):
    highest = lax.Precision.HIGHEST
    row_count = fields.shape[0]
    mesh_count = lax.axis_size("mesh")
    tile_count = lax.axis_size("tile")
    groups = mesh_count * tile_count
    slot_count = 2 * row_count // groups
    feat_width = encode_weight.shape[1]
    patch_rows = MA
    patch_cols = MB
    nodes_local = patch_rows * patch_cols
    coarse_count = CPD * groups
    target = owner_group[:, 0]
    group_onehot = (target[:, None] == jnp.arange(groups, dtype=jnp.int32)[None, :]).astype(
        jnp.int32
    )
    earlier = jnp.cumsum(group_onehot, axis=0) - group_onehot
    position = target * slot_count + jnp.sum(earlier * group_onehot, axis=1)
    matches = jnp.arange(groups * slot_count, dtype=jnp.int32)[:, None] == position[None, :]
    dispatch = matches.astype(jnp.bfloat16)
    slot_node = (jnp.max(jnp.where(matches, owner_node[None, :] + 1, 0), axis=1) - 1).reshape(
        groups, slot_count
    )
    pre_encode = jnp.dot(fields, encode_weight, preferred_element_type=jnp.float32)
    hidden = jax.nn.silu(pre_encode).astype(jnp.bfloat16)
    outgoing = jnp.dot(dispatch, hidden, preferred_element_type=jnp.float32).astype(jnp.bfloat16)
    incoming, incoming_node = send_rows(outgoing.reshape(groups, slot_count, feat_width), slot_node)
    node_match = (
        incoming_node[:, None] == jnp.arange(nodes_local, dtype=jnp.int32)[None, :]
    ).astype(jnp.bfloat16)
    node_in = jnp.einsum(
        "sn,sh->nh", node_match, incoming, preferred_element_type=jnp.float32
    ).astype(jnp.bfloat16)
    counts = jnp.sum(
        (stencil_codes[:, :, None] == jnp.arange(25, dtype=jnp.int32)[None, None, :]).astype(
            jnp.float32
        ),
        axis=1,
    )
    counts = counts.astype(jnp.bfloat16).reshape(patch_rows, patch_cols, 25)
    padded_nodes, padded_counts = (
        padded(node_in.reshape(patch_rows, patch_cols, feat_width), (("mesh", 0), ("tile", 1)), 2),
        padded(counts, (("mesh", 0), ("tile", 1)), 2),
    )
    gathered = jnp.zeros((patch_rows, patch_cols, feat_width), jnp.float32)
    for code_index in range(25):
        step_x = code_index // 5 - 2
        step_y = code_index % 5 - 2
        weight_here = padded_counts[
            2 : 2 + patch_rows, 2 : 2 + patch_cols, code_index : code_index + 1
        ].astype(jnp.float32)
        gathered = gathered + weight_here * padded_nodes[
            2 + step_x : 2 + step_x + patch_rows, 2 + step_y : 2 + step_y + patch_cols
        ].astype(jnp.float32)
    agg = gathered.reshape(nodes_local, feat_width).astype(jnp.bfloat16)
    agg_full = lax.all_gather(agg, "feat", axis=1, tiled=True)
    pre_mesh = jnp.dot(agg_full, process_weight, preferred_element_type=jnp.float32)
    level_one = node_in.astype(jnp.float32) + jax.nn.silu(pre_mesh)
    coarse_match = (
        coarse_ids[:, None] == jnp.arange(coarse_count, dtype=jnp.int32)[None, :]
    ).astype(jnp.float32)
    coarse_part = jnp.dot(coarse_match.T, level_one, precision=highest)
    coarse_total = lax.psum(coarse_part, ("mesh", "tile"))
    coarse_in = lax.all_gather(coarse_total.astype(jnp.bfloat16), "feat", axis=1, tiled=True)
    pre_coarse = jnp.dot(coarse_in, coarse_weight, preferred_element_type=jnp.float32)
    coarse_out = jax.nn.silu(pre_coarse).astype(jnp.bfloat16)
    level_two = (
        level_one
        + jnp.dot(coarse_match.astype(jnp.bfloat16), coarse_out, preferred_element_type=jnp.float32)
    ).astype(jnp.bfloat16)
    reply_rows = jnp.dot(node_match, level_two, preferred_element_type=jnp.float32).astype(
        jnp.bfloat16
    )
    returned = route_block(reply_rows, mesh_count, tile_count, "reply")
    merged = (
        hidden.astype(jnp.float32)
        + jnp.einsum("sr,sh->rh", dispatch, returned, preferred_element_type=jnp.float32)
    ).astype(jnp.bfloat16)
    pred_part = jnp.dot(merged, decode_weight, preferred_element_type=jnp.float32)
    prediction = lax.psum(pred_part, "feat")
    decode_grad = jnp.dot(merged.astype(jnp.float32).T, cotangent, precision=highest)
    grad_merged = jnp.dot(cotangent, decode_weight.astype(jnp.float32).T, precision=highest)
    grad_out = jnp.dot(
        dispatch, grad_merged.astype(jnp.bfloat16), preferred_element_type=jnp.float32
    ).astype(jnp.bfloat16)
    grad_in = route_block(grad_out, mesh_count, tile_count, "gradient")
    grad_two = jnp.einsum("sn,sh->nh", node_match, grad_in, preferred_element_type=jnp.float32)
    coarse_grad_part = jnp.dot(coarse_match.T, grad_two, precision=highest)
    grad_coarse_out = lax.psum(coarse_grad_part, ("mesh", "tile"))
    grad_pre_coarse = grad_coarse_out * silu_grad(pre_coarse)
    coarse_grad = jnp.dot(coarse_in.astype(jnp.float32).T, grad_pre_coarse, precision=highest)
    grad_coarse_full = jnp.dot(
        grad_pre_coarse, coarse_weight.astype(jnp.float32).T, precision=highest
    )
    grad_coarse_in = lax.psum_scatter(grad_coarse_full, "feat", scatter_dimension=1, tiled=True)
    grad_one = grad_two + jnp.dot(coarse_match, grad_coarse_in, precision=highest)
    grad_pre_mesh = grad_one * silu_grad(pre_mesh)
    process_grad = jnp.dot(agg_full.astype(jnp.float32).T, grad_pre_mesh, precision=highest)
    grad_pre_full = lax.all_gather(grad_pre_mesh, "feat", axis=1, tiled=True)
    weight_full = lax.all_gather(process_weight, "feat", axis=1, tiled=True)
    own_rows = lax.dynamic_slice_in_dim(
        weight_full, lax.axis_index("feat") * feat_width, feat_width, 0
    )
    grad_agg = jnp.dot(grad_pre_full, own_rows.astype(jnp.float32).T, precision=highest).astype(
        jnp.bfloat16
    )
    padded_grad = padded(
        grad_agg.reshape(patch_rows, patch_cols, feat_width), (("mesh", 0), ("tile", 1)), 2
    )
    spread = jnp.zeros((patch_rows, patch_cols, feat_width), jnp.float32)
    for code_index in range(25):
        step_x = code_index // 5 - 2
        step_y = code_index % 5 - 2
        weight_there = padded_counts[
            2 - step_x : 2 - step_x + patch_rows,
            2 - step_y : 2 - step_y + patch_cols,
            code_index : code_index + 1,
        ].astype(jnp.float32)
        spread = spread + weight_there * padded_grad[
            2 - step_x : 2 - step_x + patch_rows, 2 - step_y : 2 - step_y + patch_cols
        ].astype(jnp.float32)
    grad_zero = (grad_one + spread.reshape(nodes_local, feat_width)).astype(jnp.bfloat16)
    back_rows = jnp.dot(node_match, grad_zero, preferred_element_type=jnp.float32).astype(
        jnp.bfloat16
    )
    grad_back = route_block(back_rows, mesh_count, tile_count, "return")
    grad_hidden = grad_merged + jnp.einsum(
        "sr,sh->rh", dispatch, grad_back, preferred_element_type=jnp.float32
    )
    grad_pre_encode = grad_hidden * silu_grad(pre_encode)
    encode_grad = jnp.dot(fields.astype(jnp.float32).T, grad_pre_encode, precision=highest)
    encode_grad, process_grad, decode_grad = lax.psum(
        (encode_grad, process_grad, decode_grad), ("mesh", "tile")
    )
    return (prediction, encode_grad, process_grad, coarse_grad, decode_grad)


def body(fields, owner_group, owner_node, stencil_codes, *rest):
    groups = lax.axis_size("mesh") * lax.axis_size("tile")
    rows, c_in = fields.shape
    cells, nodes = groups * rows, groups * MA * MB
    degree = stencil_codes.shape[1]
    fits = (
        lax.axis_size("mesh") > 2
        and cells * nodes <= REPLICATE_LIMIT
        and lax.axis_size("feat") == 2
        and rows == c_in == rest[-1].shape[1]
        and max(nodes, 25) <= 256
        and degree + 3 <= ID_ROWS
        and MA * MB <= rows
    )
    plan = replicated if fits else distributed
    return plan(fields, owner_group, owner_node, stencil_codes, *rest)


def solution(mesh):
    placed = (
        P(("parts", "mesh", "tile"), None),
        P(("mesh", "tile"), None),
        P(("mesh", "tile")),
        P(("mesh", "tile"), None),
        P(("mesh", "tile")),
        P(None, "feat"),
        P(None, "feat"),
        P(None, "feat"),
        P("feat", None),
        P(("parts", "mesh", "tile"), None),
    )
    return jax.shard_map(
        body,
        mesh=mesh,
        in_specs=placed,
        out_specs=(
            P(("parts", "mesh", "tile"), None),
            P("parts", "feat"),
            P("parts", "feat"),
            P("parts", "feat"),
            P(("parts", "feat"), None),
        ),
        check_vma=False,
    )
```

```python
import functools

import jax
import jax.numpy as jnp
from jax import lax
from jax.experimental import pallas as pl
from jax.experimental.pallas import tpu as pltpu
from jax.sharding import PartitionSpec as P


MA = 4
MB = 8
CPD = 2
ID_ROWS = 16
EARLY = 3
GRANT = 20 << 20
REPLICATE_LIMIT = 1 << 20

F32 = jnp.float32
BF16 = jnp.bfloat16
NN = (((1,), (0,)), ((), ()))
NT = (((1,), (1,)), ((), ()))
TN = (((0,), (0,)), ((), ()))


def mm(lhs, rhs, dims=NN):
    return lax.dot_general(lhs, rhs, dims, preferred_element_type=F32)


def split(value):
    high = value.astype(BF16)
    return high, (value - high.astype(F32)).astype(BF16)


def held(value):
    return pltpu.with_memory_space_constraint(value, pltpu.VMEM)


def pack_kernel(fields, group_row, node_row, codes, coarse_row, cotangent, out, wide):
    rows = fields.shape[0]
    degree, local = codes.shape
    core = lax.axis_index("feat")

    @pl.when(core == 0)
    def _():
        out[0:rows, :] = fields[...]

    @pl.when(core != 0)
    def _():
        out[0:rows, :] = cotangent[...].astype(BF16)

    wide[...] = jnp.zeros(wide.shape, F32)
    wide[0:1, :] = group_row[...].astype(F32)
    wide[1:2, :] = node_row[...].astype(F32)
    wide[2 : 2 + degree, 0:local] = codes[...].astype(F32)
    wide[2 + degree : 3 + degree, 0:local] = coarse_row[...].astype(F32)
    out[rows : rows + ID_ROWS, :] = wide[...].astype(BF16)


def tags_at(ref, start):
    tags = ref[pl.ds(start, ID_ROWS), :].astype(F32)
    return tags, jnp.transpose(tags)


def hits(tags, tags_t, nodes):
    local = MA * MB
    rows = tags.shape[1]
    sub = lax.broadcasted_iota(jnp.int32, (nodes, rows), 0).astype(F32)
    lane = lax.broadcasted_iota(jnp.int32, (rows, nodes), 1).astype(F32)
    by_node = (sub == tags[0:1, :] * local + tags[1:2, :]).astype(BF16)
    by_cell = (lane == tags_t[:, 0:1] * local + tags_t[:, 1:2]).astype(BF16)
    return by_node, by_cell


def near_kernel(
    groups,
    near,
    far,
    we_own,
    we_oth,
    wd_own,
    node_part,
    cot_part,
    dec_part,
    hid_own,
    slope,
    hit_t,
    cells,
    gm,
    hit,
    cots,
    hid,
):
    nodes = groups * MA * MB
    rows, width = hid_own.shape[0], we_own.shape[1]
    block = rows + ID_ROWS
    core = lax.axis_index("feat")
    for p in range(near.shape[0] // block):
        span = slice(p * rows, (p + 1) * rows)
        here = pl.ds(p * block, rows)
        hit[:, span], hit_t[span, :] = hits(*tags_at(near, p * block + rows), nodes)
        a, b = near[here, :], far[here, :]
        cell = jnp.where(core == 0, a, b)
        cells[span, :] = cell
        cots[span, :] = jnp.where(core == 0, b, a)
        pre = mm(cell, we_own[...])
        sig = jax.nn.sigmoid(pre)
        act = pre * sig
        hid[span, 0:width] = act.astype(BF16)
        slope[span, :] = sig + act * (1.0 - sig)
        pre = mm(cell, we_oth[...])
        hid[span, width:] = (pre * jax.nn.sigmoid(pre)).astype(BF16)
    cot = cots[...]
    hid_own[...] = hid[0:rows, :]
    node_part[...] = mm(hit[...], hid[...])
    cot_part[...] = mm(hit[...], cot)
    dec_part[...] = mm(hid[:, :width], cot, TN)
    gm[...] = mm(cot, wd_own[...], NT)


def index_kernel(
    shifts, tile_count, degree, near, rest, hit, hit_t, reach_out, member_out, ids
):
    mesh_count = len(shifts)
    groups = mesh_count * tile_count
    local = MA * MB
    nodes = groups * local
    block = (near.shape[0] + rest.shape[0]) // groups
    count = near.shape[0] // block
    rows = block - ID_ROWS
    my_mesh = lax.axis_index("mesh")
    my_tile = lax.axis_index("tile")
    for p in range(groups):
        shift, turn = shifts[p // tile_count], p % tile_count
        group = lax.rem(my_mesh - shift + mesh_count, mesh_count) * tile_count + lax.rem(
            my_tile - turn + tile_count, tile_count
        )
        q = p - count
        tags, tags_t = tags_at(near, p * block + rows) if q < 0 else tags_at(rest, q * block + rows)
        if q >= 0:
            span = slice(q * rows, (q + 1) * rows)
            hit[:, span], hit_t[span, :] = hits(tags, tags_t, nodes)
        ids[pl.ds(pl.multiple_of(group * local, local), local), :] = tags_t[0:local, :]

    tags = ids[...].astype(jnp.int32)
    index = lax.broadcasted_iota(jnp.int32, (nodes, ID_ROWS), 0)
    group, place = lax.div(index, local), lax.rem(index, local)
    row = lax.div(group, tile_count) * MA + lax.div(place, MB)
    col = lax.rem(group, tile_count) * MB + lax.rem(place, MB)
    tall, broad = mesh_count * MA, tile_count * MB
    row = lax.rem(row + lax.div(tags, 5) - 2 + tall, tall)
    col = lax.rem(col + lax.rem(tags, 5) - 2 + broad, broad)
    peer = (lax.div(row, MA) * tile_count + lax.div(col, MB)) * local
    peer = peer + lax.rem(row, MA) * MB + lax.rem(col, MB)
    over = lax.broadcasted_iota(jnp.int32, (nodes, nodes), 1)
    reach = jnp.zeros((nodes, nodes), F32)
    for k in range(2, 2 + degree):
        reach = reach + (over == peer[:, k : k + 1]).astype(F32)
    reach_out[...] = reach.astype(BF16)
    member_out[...] = (
        lax.broadcasted_iota(jnp.int32, (nodes, CPD * groups), 1)
        == tags[:, 2 + degree : 3 + degree]
    ).astype(BF16)


def step_kernel(
    near_count,
    rest,
    far,
    node_part,
    cot_part,
    dec_part,
    hid_own,
    slope_near,
    hit_t_near,
    cells_near,
    gm_near,
    hit,
    hit_t,
    reach_ref,
    member_ref,
    we_own,
    wp_own,
    wc_own,
    wd_own,
    we_oth,
    wp_oth,
    wc_oth,
    wd_oth,
    prediction_out,
    encode_out,
    process_out,
    coarse_out,
    decode_out,
    cells,
    cots,
    hid,
    slope,
    gpe,
    gpe_near,
    gm,
    prediction,
    encode_grad,
    process_grad,
    coarse_grad,
    decode_grad,
    sems,
):
    rows, width = hid_own.shape[0], we_own.shape[1]
    block = rows + ID_ROWS
    count = rest.shape[0] // block
    core = lax.axis_index("feat")
    own = pl.ds(pl.multiple_of(core * width, width), width)
    oth = pl.ds(pl.multiple_of((1 - core) * width, width), width)
    pairs = (
        (prediction, prediction_out),
        (encode_grad, encode_out),
        (process_grad, process_out),
        (coarse_grad, coarse_out),
        (decode_grad, decode_out),
    )

    def half_copy(i, half):
        source, target = pairs[i]
        size = source.shape[0] // 2
        part = pl.ds(pl.multiple_of(half * size, size), size)
        return pltpu.make_async_copy(source.at[part], target.at[part], sems.at[i, half])

    def launch(*chosen):
        def start(half, carry):
            for i in chosen:
                half_copy(i, half).start()
            return carry

        lax.fori_loop(0, 2, start, 0)

    for p in range(count):
        here = pl.ds(p * block, rows)
        span = slice(p * rows, (p + 1) * rows)
        a, b = rest[here, :], far[here, :]
        cell = jnp.where(core == 0, a, b)
        cells[span, :] = cell
        cots[span, :] = jnp.where(core == 0, b, a)
        pre = mm(cell, we_own[...])
        sig = jax.nn.sigmoid(pre)
        act = pre * sig
        hid[span, 0:width] = act.astype(BF16)
        slope[span, :] = sig + act * (1.0 - sig)
        pre = mm(cell, we_oth[...])
        hid[span, width:] = (pre * jax.nn.sigmoid(pre)).astype(BF16)

    reach = reach_ref[...]
    member = member_ref[...]
    node_in = (node_part[...] + mm(hit[...], hid[...])).astype(BF16)
    agg = mm(reach, node_in).astype(BF16)
    agg_own, agg_oth = agg[:, :width], agg[:, width:]
    pre_mesh = (
        mm(agg_own, wp_own[own, :]) + mm(agg_oth, wp_own[oth, :]),
        mm(agg_own, wp_oth[own, :]) + mm(agg_oth, wp_oth[oth, :]),
    )
    sig_mesh = tuple(jax.nn.sigmoid(v) for v in pre_mesh)
    act_mesh = tuple(v * s for v, s in zip(pre_mesh, sig_mesh))
    level_one = (
        node_in[:, :width].astype(F32) + act_mesh[0],
        node_in[:, width:].astype(F32) + act_mesh[1],
    )
    coarse_in = []
    for v in level_one:
        high, low = split(v)
        coarse_in.append((mm(member, high, TN) + mm(member, low, TN)).astype(BF16))
    pre_coarse = (
        mm(coarse_in[0], wc_own[own, :]) + mm(coarse_in[1], wc_own[oth, :]),
        mm(coarse_in[0], wc_oth[own, :]) + mm(coarse_in[1], wc_oth[oth, :]),
    )
    sig_coarse = tuple(jax.nn.sigmoid(v) for v in pre_coarse)
    act_coarse = tuple(v * s for v, s in zip(pre_coarse, sig_coarse))
    level_two = tuple(
        (v + mm(member, c.astype(BF16))).astype(BF16) for v, c in zip(level_one, act_coarse)
    )
    cot = cots[...]
    node_cot = cot_part[...] + mm(hit[...], cot)
    cot_high, cot_low = split(node_cot)
    grad_two = tuple(mm(cot_high, w[...], NT) + mm(cot_low, w[...], NT) for w in (wd_own, wd_oth))
    gpc = []
    for g, s, c in zip(grad_two, sig_coarse, act_coarse):
        high, low = split(g)
        total = mm(member, high, TN) + mm(member, low, TN)
        gpc.append((total * (s + c * (1.0 - s))).astype(BF16))
    coarse_grad[own, :] = mm(coarse_in[0], gpc[0], TN)
    coarse_grad[oth, :] = mm(coarse_in[1], gpc[0], TN)


    grad_coarse_in = (
        mm(gpc[0], wc_own[own, :], NT) + mm(gpc[1], wc_oth[own, :], NT),
        mm(gpc[0], wc_own[oth, :], NT) + mm(gpc[1], wc_oth[oth, :], NT),
    )
    grad_one = tuple(g + mm(member, c.astype(BF16)) for g, c in zip(grad_two, grad_coarse_in))
    gpm = tuple(
        (g * (s + c * (1.0 - s))).astype(BF16) for g, s, c in zip(grad_one, sig_mesh, act_mesh)
    )
    process_grad[own, :] = mm(agg_own, gpm[0], TN)
    process_grad[oth, :] = mm(agg_oth, gpm[0], TN)

    launch(2, 3)
    gm[...] = mm(cot, wd_own[...], NT)
    mine = hit_t_near[0:rows, :]
    merged = (
        (hid_own[:, :width].astype(F32) + mm(mine, level_two[0])).astype(BF16),
        (hid_own[:, width:].astype(F32) + mm(mine, level_two[1])).astype(BF16),
    )
    prediction[...] = mm(merged[0], wd_own[...]) + mm(merged[1], wd_oth[...])

    decode_grad[...] = (
        dec_part[...] + mm(hid[:, :width], cot, TN) + mm(level_two[0], cot_high, TN)
    )

    grad_agg = (mm(gpm[0], wp_own[own, :], NT) + mm(gpm[1], wp_oth[own, :], NT)).astype(BF16)
    grad_zero = (grad_one[0] + mm(reach, grad_agg, TN)).astype(BF16)
    for p in range(count):
        span = slice(p * rows, (p + 1) * rows)
        grad_hidden = gm[span, :] + mm(hit_t[span, :], grad_zero)
        gpe[span, :] = (grad_hidden * slope[span, :]).astype(BF16)
    for p in range(near_count):
        span = slice(p * rows, (p + 1) * rows)
        grad_hidden = gm_near[span, :] + mm(hit_t_near[span, :], grad_zero)
        gpe_near[span, :] = (grad_hidden * slope_near[span, :]).astype(BF16)
    encode_grad[...] = mm(cells[...], gpe[...], TN) + mm(cells_near[...], gpe_near[...], TN)
    for i in (0, 1, 4):
        for half in range(2):
            half_copy(i, half).start()
    for i in range(len(pairs)):
        for half in range(2):
            half_copy(i, half).wait()


def replicated(
    fields,
    owner_group,
    owner_node,
    stencil_codes,
    coarse_ids,
    encode_weight,
    process_weight,
    coarse_weight,
    decode_weight,
    cotangent,
):
    mesh_count = lax.axis_size("mesh")
    tile_count = lax.axis_size("tile")
    groups = mesh_count * tile_count
    rows, c_in = fields.shape
    c_out = cotangent.shape[1]
    width = encode_weight.shape[1]
    nodes = groups * MA * MB
    block = rows + ID_ROWS
    weights = (encode_weight, process_weight, coarse_weight, decode_weight)
    swap = [(0, 1), (1, 0)]
    vmem = pl.BlockSpec(memory_space=pltpu.VMEM)
    hbm = pl.BlockSpec(memory_space=pl.ANY)
    grant = pltpu.CompilerParams(vmem_limit_bytes=GRANT)
    payload = pl.pallas_call(
        pack_kernel,
        in_specs=[vmem] * 6,
        out_specs=vmem,
        out_shape=pltpu.VMEM((block, c_in), BF16),
        scratch_shapes=[pltpu.VMEM((ID_ROWS, rows), F32)],
    )(
        fields,
        owner_group.reshape(1, rows),
        owner_node.reshape(1, rows),
        stencil_codes.T,
        coarse_ids.reshape(1, MA * MB),
        cotangent,
    )
    columns = [payload]
    for turn in range(1, tile_count):
        ring = [(i, (i + turn) % tile_count) for i in range(tile_count)]
        columns.append(lax.ppermute(payload, "tile", ring))
    near = jnp.concatenate(columns, axis=0)
    near, weights = lax.optimization_barrier((near, weights))
    shifts = [0, EARLY, *[i for i in range(1, mesh_count) if i != EARLY]]
    blocks = [near]
    for shift in shifts[1:]:
        ring = [(i, (i + shift) % mesh_count) for i in range(mesh_count)]
        blocks.append(lax.ppermute(near, "mesh", ring))
    near_far = lax.ppermute(near, "feat", swap)
    others = tuple(lax.ppermute(w, "feat", swap) for w in weights)
    early_far = lax.ppermute(blocks[1], "feat", swap)
    near = jnp.concatenate(blocks[:2], axis=0)
    near_far = jnp.concatenate([near_far, early_far], axis=0)
    degree = stencil_codes.shape[1]
    beside = 2 * tile_count * rows
    near_call = pl.pallas_call(
        functools.partial(near_kernel, groups),
        in_specs=[vmem] * 5,
        compiler_params=grant,
        out_specs=[vmem] * 8,
        out_shape=(
            pltpu.VMEM((nodes, 2 * width), F32),
            pltpu.VMEM((nodes, c_out), F32),
            pltpu.VMEM((width, c_out), F32),
            pltpu.VMEM((rows, 2 * width), BF16),
            pltpu.VMEM((beside, width), F32),
            pltpu.VMEM((beside, nodes), BF16),
            pltpu.VMEM((beside, c_in), BF16),
            pltpu.VMEM((beside, width), F32),
        ),
        scratch_shapes=[
            pltpu.VMEM((nodes, beside), BF16),
            pltpu.VMEM((beside, c_out), BF16),
            pltpu.VMEM((beside, 2 * width), BF16),
        ],
    )
    parts = near_call(*map(held, (near, near_far, encode_weight, others[0], decode_weight)))
    rest = jnp.concatenate(blocks[2:], axis=0)
    rest_far = lax.ppermute(rest, "feat", swap)
    cells = (groups - 2 * tile_count) * rows
    tables = pl.pallas_call(
        functools.partial(index_kernel, shifts, tile_count, degree),
        in_specs=[vmem] * 2,
        compiler_params=grant,
        out_specs=[vmem] * 4,
        out_shape=(
            pltpu.VMEM((nodes, cells), BF16),
            pltpu.VMEM((cells, nodes), BF16),
            pltpu.VMEM((nodes, nodes), BF16),
            pltpu.VMEM((nodes, CPD * groups), BF16),
        ),
        scratch_shapes=[pltpu.VMEM((nodes, ID_ROWS), F32)],
    )(held(near), held(rest))
    outs = (
        jax.ShapeDtypeStruct((rows, c_out), F32),
        jax.ShapeDtypeStruct((c_in, width), F32),
        jax.ShapeDtypeStruct(process_weight.shape, F32),
        jax.ShapeDtypeStruct(coarse_weight.shape, F32),
        jax.ShapeDtypeStruct((width, c_out), F32),
    )
    operands = [held(v) for v in (rest, rest_far, *parts, *tables, *weights, *others)]
    return pl.pallas_call(
        functools.partial(step_kernel, 2 * tile_count),
        in_specs=[vmem] * len(operands),
        compiler_params=grant,
        out_specs=[hbm] * 5,
        out_shape=outs,
        scratch_shapes=[
            pltpu.VMEM((cells, c_in), BF16),
            pltpu.VMEM((cells, c_out), BF16),
            pltpu.VMEM((cells, 2 * width), BF16),
            pltpu.VMEM((cells, width), F32),
            pltpu.VMEM((cells, width), BF16),
            pltpu.VMEM((beside, width), BF16),
            pltpu.VMEM((cells, width), F32),
            *[pltpu.VMEM(o.shape, F32) for o in outs],
            pltpu.SemaphoreType.DMA((5, 2)),
        ],
    )(*operands)


def padded(array, sides, width):
    for axis, dim in sides:
        peers, length = (lax.axis_size(axis), array.shape[dim])
        up = [(i, (i + 1) % peers) for i in range(peers)]
        down = [(j, i) for i, j in up]
        last = lax.slice_in_dim(array, length - width, length, axis=dim)
        initial = lax.slice_in_dim(array, 0, width, axis=dim)
        before = lax.ppermute(last, axis, up)
        after = lax.ppermute(initial, axis, down)
        array = jnp.concatenate([before, array, after], axis=dim)
    return array


def silu_grad(pre):
    sig = jax.nn.sigmoid(pre)
    return sig * (1.0 + pre * (1.0 - sig))


def send_rows(outgoing, slot_node):
    feat_width = outgoing.shape[-1]
    got, got_node = (
        lax.all_to_all(outgoing, ("mesh", "tile"), split_axis=0, concat_axis=0, tiled=True),
        lax.all_to_all(slot_node, ("mesh", "tile"), split_axis=0, concat_axis=0, tiled=True),
    )
    return (got.reshape(-1, feat_width), got_node.reshape(-1))


def route_block(block, mesh_count, tile_count, purpose):
    feat_width = block.shape[-1]
    slot_count = block.shape[0] // (mesh_count * tile_count)
    flat_shape = (mesh_count * tile_count, slot_count, feat_width)
    if purpose == "reply":
        moved = lax.all_to_all(
            block.reshape(flat_shape), ("mesh", "tile"), split_axis=0, concat_axis=0, tiled=True
        )
    elif purpose == "gradient":
        moved = lax.all_to_all(
            block.reshape(flat_shape), ("mesh", "tile"), split_axis=0, concat_axis=0, tiled=True
        )
    else:
        moved = lax.all_to_all(
            block.reshape(flat_shape), ("mesh", "tile"), split_axis=0, concat_axis=0, tiled=True
        )
    return moved.reshape(-1, feat_width)


def distributed(
    fields,
    owner_group,
    owner_node,
    stencil_codes,
    coarse_ids,
    encode_weight,
    process_weight,
    coarse_weight,
    decode_weight,
    cotangent,
):
    highest = lax.Precision.HIGHEST
    row_count = fields.shape[0]
    mesh_count = lax.axis_size("mesh")
    tile_count = lax.axis_size("tile")
    groups = mesh_count * tile_count
    slot_count = 2 * row_count // groups
    feat_width = encode_weight.shape[1]
    patch_rows = MA
    patch_cols = MB
    nodes_local = patch_rows * patch_cols
    coarse_count = CPD * groups
    target = owner_group[:, 0]
    group_onehot = (target[:, None] == jnp.arange(groups, dtype=jnp.int32)[None, :]).astype(
        jnp.int32
    )
    earlier = jnp.cumsum(group_onehot, axis=0) - group_onehot
    position = target * slot_count + jnp.sum(earlier * group_onehot, axis=1)
    matches = jnp.arange(groups * slot_count, dtype=jnp.int32)[:, None] == position[None, :]
    dispatch = matches.astype(jnp.bfloat16)
    slot_node = (jnp.max(jnp.where(matches, owner_node[None, :] + 1, 0), axis=1) - 1).reshape(
        groups, slot_count
    )
    pre_encode = jnp.dot(fields, encode_weight, preferred_element_type=jnp.float32)
    hidden = jax.nn.silu(pre_encode).astype(jnp.bfloat16)
    outgoing = jnp.dot(dispatch, hidden, preferred_element_type=jnp.float32).astype(jnp.bfloat16)
    incoming, incoming_node = send_rows(outgoing.reshape(groups, slot_count, feat_width), slot_node)
    node_match = (
        incoming_node[:, None] == jnp.arange(nodes_local, dtype=jnp.int32)[None, :]
    ).astype(jnp.bfloat16)
    node_in = jnp.einsum(
        "sn,sh->nh", node_match, incoming, preferred_element_type=jnp.float32
    ).astype(jnp.bfloat16)
    counts = jnp.sum(
        (stencil_codes[:, :, None] == jnp.arange(25, dtype=jnp.int32)[None, None, :]).astype(
            jnp.float32
        ),
        axis=1,
    )
    counts = counts.astype(jnp.bfloat16).reshape(patch_rows, patch_cols, 25)
    padded_nodes, padded_counts = (
        padded(node_in.reshape(patch_rows, patch_cols, feat_width), (("mesh", 0), ("tile", 1)), 2),
        padded(counts, (("mesh", 0), ("tile", 1)), 2),
    )
    gathered = jnp.zeros((patch_rows, patch_cols, feat_width), jnp.float32)
    for code_index in range(25):
        step_x = code_index // 5 - 2
        step_y = code_index % 5 - 2
        weight_here = padded_counts[
            2 : 2 + patch_rows, 2 : 2 + patch_cols, code_index : code_index + 1
        ].astype(jnp.float32)
        gathered = gathered + weight_here * padded_nodes[
            2 + step_x : 2 + step_x + patch_rows, 2 + step_y : 2 + step_y + patch_cols
        ].astype(jnp.float32)
    agg = gathered.reshape(nodes_local, feat_width).astype(jnp.bfloat16)
    agg_full = lax.all_gather(agg, "feat", axis=1, tiled=True)
    pre_mesh = jnp.dot(agg_full, process_weight, preferred_element_type=jnp.float32)
    level_one = node_in.astype(jnp.float32) + jax.nn.silu(pre_mesh)
    coarse_match = (
        coarse_ids[:, None] == jnp.arange(coarse_count, dtype=jnp.int32)[None, :]
    ).astype(jnp.float32)
    coarse_part = jnp.dot(coarse_match.T, level_one, precision=highest)
    coarse_total = lax.psum(coarse_part, ("mesh", "tile"))
    coarse_in = lax.all_gather(coarse_total.astype(jnp.bfloat16), "feat", axis=1, tiled=True)
    pre_coarse = jnp.dot(coarse_in, coarse_weight, preferred_element_type=jnp.float32)
    coarse_out = jax.nn.silu(pre_coarse).astype(jnp.bfloat16)
    level_two = (
        level_one
        + jnp.dot(coarse_match.astype(jnp.bfloat16), coarse_out, preferred_element_type=jnp.float32)
    ).astype(jnp.bfloat16)
    reply_rows = jnp.dot(node_match, level_two, preferred_element_type=jnp.float32).astype(
        jnp.bfloat16
    )
    returned = route_block(reply_rows, mesh_count, tile_count, "reply")
    merged = (
        hidden.astype(jnp.float32)
        + jnp.einsum("sr,sh->rh", dispatch, returned, preferred_element_type=jnp.float32)
    ).astype(jnp.bfloat16)
    pred_part = jnp.dot(merged, decode_weight, preferred_element_type=jnp.float32)
    prediction = lax.psum(pred_part, "feat")
    decode_grad = jnp.dot(merged.astype(jnp.float32).T, cotangent, precision=highest)
    grad_merged = jnp.dot(cotangent, decode_weight.astype(jnp.float32).T, precision=highest)
    grad_out = jnp.dot(
        dispatch, grad_merged.astype(jnp.bfloat16), preferred_element_type=jnp.float32
    ).astype(jnp.bfloat16)
    grad_in = route_block(grad_out, mesh_count, tile_count, "gradient")
    grad_two = jnp.einsum("sn,sh->nh", node_match, grad_in, preferred_element_type=jnp.float32)
    coarse_grad_part = jnp.dot(coarse_match.T, grad_two, precision=highest)
    grad_coarse_out = lax.psum(coarse_grad_part, ("mesh", "tile"))
    grad_pre_coarse = grad_coarse_out * silu_grad(pre_coarse)
    coarse_grad = jnp.dot(coarse_in.astype(jnp.float32).T, grad_pre_coarse, precision=highest)
    grad_coarse_full = jnp.dot(
        grad_pre_coarse, coarse_weight.astype(jnp.float32).T, precision=highest
    )
    grad_coarse_in = lax.psum_scatter(grad_coarse_full, "feat", scatter_dimension=1, tiled=True)
    grad_one = grad_two + jnp.dot(coarse_match, grad_coarse_in, precision=highest)
    grad_pre_mesh = grad_one * silu_grad(pre_mesh)
    process_grad = jnp.dot(agg_full.astype(jnp.float32).T, grad_pre_mesh, precision=highest)
    grad_pre_full = lax.all_gather(grad_pre_mesh, "feat", axis=1, tiled=True)
    weight_full = lax.all_gather(process_weight, "feat", axis=1, tiled=True)
    own_rows = lax.dynamic_slice_in_dim(
        weight_full, lax.axis_index("feat") * feat_width, feat_width, 0
    )
    grad_agg = jnp.dot(grad_pre_full, own_rows.astype(jnp.float32).T, precision=highest).astype(
        jnp.bfloat16
    )
    padded_grad = padded(
        grad_agg.reshape(patch_rows, patch_cols, feat_width), (("mesh", 0), ("tile", 1)), 2
    )
    spread = jnp.zeros((patch_rows, patch_cols, feat_width), jnp.float32)
    for code_index in range(25):
        step_x = code_index // 5 - 2
        step_y = code_index % 5 - 2
        weight_there = padded_counts[
            2 - step_x : 2 - step_x + patch_rows,
            2 - step_y : 2 - step_y + patch_cols,
            code_index : code_index + 1,
        ].astype(jnp.float32)
        spread = spread + weight_there * padded_grad[
            2 - step_x : 2 - step_x + patch_rows, 2 - step_y : 2 - step_y + patch_cols
        ].astype(jnp.float32)
    grad_zero = (grad_one + spread.reshape(nodes_local, feat_width)).astype(jnp.bfloat16)
    back_rows = jnp.dot(node_match, grad_zero, preferred_element_type=jnp.float32).astype(
        jnp.bfloat16
    )
    grad_back = route_block(back_rows, mesh_count, tile_count, "return")
    grad_hidden = grad_merged + jnp.einsum(
        "sr,sh->rh", dispatch, grad_back, preferred_element_type=jnp.float32
    )
    grad_pre_encode = grad_hidden * silu_grad(pre_encode)
    encode_grad = jnp.dot(fields.astype(jnp.float32).T, grad_pre_encode, precision=highest)
    encode_grad, process_grad, decode_grad = lax.psum(
        (encode_grad, process_grad, decode_grad), ("mesh", "tile")
    )
    return (prediction, encode_grad, process_grad, coarse_grad, decode_grad)


def body(fields, owner_group, owner_node, stencil_codes, *rest):
    groups = lax.axis_size("mesh") * lax.axis_size("tile")
    rows, c_in = fields.shape
    cells, nodes = groups * rows, groups * MA * MB
    degree = stencil_codes.shape[1]
    fits = (
        lax.axis_size("mesh") > 2
        and cells * nodes <= REPLICATE_LIMIT
        and lax.axis_size("feat") == 2
        and rows == c_in == rest[-1].shape[1]
        and max(nodes, 25) <= 256
        and degree + 3 <= ID_ROWS
        and MA * MB <= rows
    )
    plan = replicated if fits else distributed
    return plan(fields, owner_group, owner_node, stencil_codes, *rest)


def solution(mesh):
    placed = (
        P(("parts", "mesh", "tile"), None),
        P(("mesh", "tile"), None),
        P(("mesh", "tile")),
        P(("mesh", "tile"), None),
        P(("mesh", "tile")),
        P(None, "feat"),
        P(None, "feat"),
        P(None, "feat"),
        P("feat", None),
        P(("parts", "mesh", "tile"), None),
    )
    return jax.shard_map(
        body,
        mesh=mesh,
        in_specs=placed,
        out_specs=(
            P(("parts", "mesh", "tile"), None),
            P("parts", "feat"),
            P("parts", "feat"),
            P("parts", "feat"),
            P(("parts", "feat"), None),
        ),
        check_vma=False,
    )
```
